32 devices in a mesh: dp: 4 (over y, x), ctx: 8 (over z, core).
Axes of the slice: x: 2, y: 2, z: 4, core: 2. Of those that a mesh axis runs over, the one named last changes fastest.
Arguments:
- query_rows: bfloat16 [4096, 2048], P(('dp', 'ctx')), may hold values from -64 to 64
- key_rows: bfloat16 [4096, 2048], P(('dp', 'ctx')), may hold values from -64 to 64
- value_rows: bfloat16 [4096, 2048], P(('dp', 'ctx')), may hold values from -6 to 6
- cotangent: bfloat16 [4096, 2048], P(('dp', 'ctx')), may hold values from -6 to 6
- query_gain: float32 [2048], replicated, may hold values from 0.5 to 5.5
- key_gain: float32 [2048], replicated, may hold values from 0.5 to 5.5
- positions: int32 [4096], P(('dp', 'ctx')), may hold values from 0 to 511, as said below
- span_start: int32 [8, 2], P('dp'), may hold values from 0 to 384, as said below
- span_length: int32 [8, 2], P('dp'), may hold values from 64 to 128
Outputs:
- output: bfloat16 [4096, 2048], P(('dp', 'ctx'))
- query_grad: bfloat16 [4096, 2048], P(('dp', 'ctx'))
- key_grad: bfloat16 [4096, 2048], P(('dp', 'ctx'))
- value_grad: bfloat16 [4096, 2048], P(('dp', 'ctx'))
- gain_grads: float32 [2, 2048], replicated
The draws below stay inside these ranges and needn't reach their ends.
Inputs may be any that keep to these rules, and one draw needn't show every extreme that they name: Within each sequence every position 0 to 511 appears once; each block's rows are two runs of 64 consecutive positions, each run in increasing order. `span_start`: the first span of a sequence starts at 128 or earlier, the second at 256 or later; spans don't intersect and end inside the sequence.
All inputs are finite; a program needn't handle non-finite values.
Results may differ from the reference program's by a relative error of at most 0.035.
The reference program's roundings to bfloat16 on the way count: a program that leaves them out, or rounds other values in their place, can miss the bound.
Values may be sent and summed in bfloat16 or wider, within the bound.
A program may use at most 128 MiB of HBM per device.

```python
import jax
import jax.numpy as jnp
from jax import lax

HEADS = 16
HEAD = 128
TOK_DEV = 128
SEQS_CTX = 2
NSPAN = 2
CYCLE = 4
LEN = 512
SPAN = 128
PIECE = 64
NSEQ = 8
ROWS = 4096
N_DP = 4


def query_base(key):
    sample_draw = jax.random.normal(jax.random.fold_in(key, 101), (ROWS, HEADS * HEAD), jnp.float32)
    return jnp.clip(sample_draw, -64.0, 64.0)


def draw_query_rows(key, part):
    return query_base(key).astype(jnp.bfloat16)


def draw_key_rows(key, part):
    fresh_keys = jax.random.normal(jax.random.fold_in(key, 201), (ROWS, HEADS * HEAD), jnp.float32)
    return jnp.clip(fresh_keys, -64.0, 64.0).astype(jnp.bfloat16)


def gain_draw(key, salt_id):
    channel = jax.random.uniform(jax.random.fold_in(key, salt_id), (HEADS, HEAD), jnp.float32, 0.6, 1.6)
    return channel.reshape(HEADS * HEAD).astype(jnp.float32)


def draw_query_gain(key, part):
    return gain_draw(key, 302)


def draw_key_gain(key, part):
    return gain_draw(key, 303)


def draw_positions(key, part):
    seq_keys = jax.random.split(jax.random.fold_in(key, 501), NSEQ)
    orders = jax.vmap(lambda single: jax.random.permutation(single, 2 * CYCLE))(seq_keys)
    orders = orders.reshape(N_DP, SEQS_CTX, CYCLE, 2)
    orders = jnp.transpose(orders, (0, 2, 1, 3))
    places = orders[..., None] * PIECE + jnp.arange(PIECE, dtype=jnp.int32)
    return places.reshape(ROWS).astype(jnp.int32)


def draw_span_start(key, part):
    first_start = jax.random.randint(jax.random.fold_in(key, 401), (NSEQ,), 0, LEN // 2 - SPAN + 1)
    second = jax.random.randint(jax.random.fold_in(key, 402), (NSEQ,), LEN // 2, LEN - SPAN + 1)
    return jnp.stack([first_start, second], axis=1).astype(jnp.int32)


def set_ends(result, rng, smallest, largest):
    extent = result.shape
    place = [jax.random.randint(jax.random.fold_in(rng, axis), (), 0, extent[axis]) for axis in range(len(extent))]
    result = result.at[tuple(place)].set(smallest)
    longest = extent.index(max(extent))
    place[longest] = (place[longest] + 1) % extent[longest]
    return result.at[tuple(place)].set(largest)


def shard_levels(key, extent, pieces, least, largest):
    factor_of, own = 1.0, jax.random.fold_in(key, 6)
    for position, shards_of in pieces:
        draws = jnp.exp(jax.random.uniform(jax.random.fold_in(own, position), (shards_of,), jnp.float32, least / len(pieces), largest / len(pieces)))
        factor_of = factor_of * jnp.repeat(draws, extent[position] // shards_of).reshape([-1 if axis == position else 1 for axis in range(len(extent))])
    return factor_of


def scatter_about(key, extent, spread, most, pieces=(), kind=jnp.bfloat16):
    array = jax.random.normal(key, extent, jnp.float32) * spread
    if len(pieces) > 0:
        array = shard_levels(key, extent, pieces, -0.22, 0.18) * array
    return jnp.clip(array, min=-most, max=most).astype(kind)


def setup_inputs(seed: int = 0) -> dict:
    splits = jax.random.split(jax.random.key(seed), 10)
    return {
        "query_rows": draw_query_rows(jax.random.fold_in(splits[9], 71), 0),
        "key_rows": draw_key_rows(jax.random.fold_in(splits[9], 71), 0),
        "value_rows": scatter_about(splits[2], (ROWS, HEADS * HEAD), 1.0, 6.0, ((0, 32),)),
        "cotangent": scatter_about(splits[3], (ROWS, HEADS * HEAD), 1.0, 6.0, ((0, 32),)),
        "query_gain": draw_query_gain(jax.random.fold_in(splits[9], 71), 0),
        "key_gain": draw_key_gain(jax.random.fold_in(splits[9], 71), 0),
        "positions": draw_positions(jax.random.fold_in(splits[9], 71), 0),
        "span_start": draw_span_start(jax.random.fold_in(splits[9], 71), 0),
        "span_length": set_ends(jax.random.randint(splits[8], (NSEQ, NSPAN), SPAN // 2, SPAN + 1), jax.random.fold_in(splits[8], 1), SPAN // 2, SPAN).astype(jnp.int32),
    }


epsilon = 1e-05
masked_score = -1e+30

def normalize(raw_rows, gain_row):
    values = raw_rows.astype(jnp.float32).reshape(raw_rows.shape[0], HEADS, HEAD)
    inverse = lax.rsqrt(lax.optimization_barrier(jnp.mean(values * values, axis=-1, keepdims=True)) + epsilon)
    unit_rows = values * inverse
    return (unit_rows, inverse, (unit_rows * gain_row.reshape(HEADS, HEAD)).astype(jnp.bfloat16))

def norm_backward(grad_normed, unit_rows, inverse, gain_row):
    grad_unit = grad_normed * gain_row.reshape(HEADS, HEAD)
    projected = lax.optimization_barrier(jnp.mean(grad_unit * unit_rows, axis=-1, keepdims=True))
    grad_raw = inverse * (grad_unit - unit_rows * projected)
    gain_part = lax.optimization_barrier(jnp.sum(grad_normed * unit_rows, axis=0)).reshape(HEADS * HEAD)
    return (grad_raw.reshape(grad_raw.shape[0], HEADS * HEAD).astype(jnp.bfloat16), gain_part)

def span_labels(places, starts, lengths):
    inside = (places[:, None] >= starts[None, :]) & (places[:, None] < starts[None, :] + lengths[None, :])
    span_ids = jnp.arange(1, starts.shape[0] + 1, dtype=jnp.int32)
    return lax.optimization_barrier(jnp.sum(jnp.where(inside, span_ids[None, :], 0), axis=1)).astype(jnp.int32)

def visible(query_places, query_labels, key_places, key_labels):
    causal = key_places[None, :] <= query_places[:, None]
    same_span = (query_labels[:, None] == key_labels[None, :]) & (query_labels[:, None] > 0)
    return causal | same_span

def to_sequences(tensor):
    trailing = tensor.shape[1:]
    shaped = tensor.reshape((N_DP, CYCLE, SEQS_CTX, TOK_DEV) + trailing)
    return jnp.swapaxes(shaped, 1, 2).reshape((NSEQ, LEN) + trailing)

def from_sequences(tensor):
    trailing = tensor.shape[2:]
    shaped = tensor.reshape((N_DP, SEQS_CTX, CYCLE, TOK_DEV) + trailing)
    return jnp.swapaxes(shaped, 1, 2).reshape((ROWS,) + trailing)

def rounded(tensor):
    return lax.optimization_barrier(tensor.astype(jnp.bfloat16)).astype(jnp.float32)

def one_sequence(packed):
    query_normed, key_normed, value_block, out_grads, places, starts, lengths = packed
    score_scale = HEAD ** (-0.5)
    labels = span_labels(places, starts, lengths)
    allowed = visible(places, labels, places, labels)

    def one_head(head_pack):
        query_float, key_float, value_float, grad_float = head_pack
        scores = jnp.einsum('qd,kd->qk', query_float, key_float) * score_scale
        scores = jnp.where(allowed, scores, masked_score)
        row_max = lax.optimization_barrier(jnp.max(scores, axis=-1, keepdims=True))
        log_total = row_max + jnp.log(lax.optimization_barrier(jnp.sum(jnp.exp(scores - row_max), axis=-1, keepdims=True)))
        attn_probs = jnp.exp(scores - log_total)
        weights = rounded(attn_probs)
        output = jnp.einsum('qk,kd->qd', weights, value_float)
        row_delta = lax.optimization_barrier(jnp.sum(rounded(output) * grad_float, axis=-1, keepdims=True))
        grad_values = jnp.einsum('qk,qd->kd', weights, grad_float).astype(jnp.bfloat16)
        prob_grads = jnp.einsum('qd,kd->qk', grad_float, value_float)
        score_grads = rounded(attn_probs * (prob_grads - row_delta))
        grad_query = jnp.einsum('qk,kd->qd', score_grads, key_float) * score_scale
        grad_keys = jnp.einsum('qk,qd->kd', score_grads, query_float) * score_scale
        return (output.astype(jnp.bfloat16), grad_values, grad_query, grad_keys)
    head_major = tuple((jnp.transpose(tensor.astype(jnp.float32), (1, 0, 2)) for tensor in (query_normed, key_normed, value_block, out_grads)))
    results = lax.map(one_head, head_major)
    return tuple((jnp.transpose(tensor, (1, 0, 2)) for tensor in results))

def reference(query_rows, key_rows, value_rows, cotangent, query_gain, key_gain, positions, span_start, span_length):
    query_unit, query_inverse, query_normed = normalize(query_rows, query_gain)
    key_unit, key_inverse, key_normed = normalize(key_rows, key_gain)
    packed = (to_sequences(query_normed), to_sequences(key_normed), to_sequences(value_rows.reshape(ROWS, HEADS, HEAD)), to_sequences(cotangent.reshape(ROWS, HEADS, HEAD)), to_sequences(positions), span_start, span_length)
    output, grad_values, grad_query, grad_keys = lax.map(one_sequence, packed)
    output = from_sequences(output).reshape(ROWS, HEADS * HEAD)
    value_grad = from_sequences(grad_values).reshape(ROWS, HEADS * HEAD)
    query_grad, query_part = norm_backward(from_sequences(grad_query), query_unit, query_inverse, query_gain)
    key_grad, key_part = norm_backward(from_sequences(grad_keys), key_unit, key_inverse, key_gain)
    gain_grads = jnp.stack([query_part, key_part])
    return (output, query_grad, key_grad, value_grad, gain_grads)
```

```python
import functools

import jax
import jax.numpy as jnp
from jax import lax
from jax.experimental import pallas as pl
from jax.experimental.pallas import tpu as pltpu
from jax.sharding import PartitionSpec as P

HEAD = 128
SEQS_CTX = 2

epsilon = 1e-05
masked_score = -1e30
MESH = pl.DeviceIdType.MESH


def flip(index, distance, count):
    result = index
    bit = 1
    while bit < count:
        if distance & bit:
            result = result + bit - 2 * bit * ((index // bit) % 2)
        bit *= 2
    return result


def unit_of(raw):
    values = raw.astype(jnp.float32)
    inverse = lax.rsqrt(jnp.mean(values * values, axis=-1, keepdims=True) + epsilon)
    return values * inverse, inverse


def norm_backward(grad_normed, unit, inverse, gain):
    grad_unit = grad_normed * gain
    projected = jnp.mean(grad_unit * unit, axis=-1, keepdims=True)
    grad_raw = inverse * (grad_unit - unit * projected)
    return grad_raw.astype(jnp.bfloat16), jnp.sum(grad_normed * unit, axis=0, keepdims=True)


def dot(left, right, left_axis, right_axis):
    return lax.dot_general(
        left,
        right,
        (((left_axis,), (right_axis,)), ((), ())),
        preferred_element_type=jnp.float32,
    )


def kernel(
    members,
    dp_count,
    per_device,
    rows,
    query_in,
    key_in,
    value_in,
    cotangent_in,
    query_gain_in,
    key_gain_in,
    positions,
    span_start_in,
    span_length_in,
    out_ref,
    query_grad_ref,
    key_grad_ref,
    value_grad_ref,
    gain_ref,
    query_gain,
    key_gain,
    span_start,
    span_length,
    small_sem,
    in_buf,
    out_buf,
    bias,
    key_normed,
    key_total,
    value_total,
    places,
    gain_part,
    plane_buf,
    group_buf,
    in_send,
    in_recv,
    back_send,
    back_recv,
    place_send,
    place_recv,
    plane_send,
    plane_recv,
    group_send,
    group_recv,
):
    dp = lax.axis_index("dp")
    ctx = lax.axis_index("ctx")
    me = ctx // SEQS_CTX
    core = ctx % SEQS_CTX
    tokens = members * rows
    plane = dp_count * SEQS_CTX
    own = dp * SEQS_CTX + core
    sources = (query_in, key_in, value_in, cotangent_in)
    results = (out_ref, query_grad_ref, key_grad_ref, value_grad_ref)
    distances = range(1, members)
    scale = HEAD ** (-0.5)

    def row_slice(member):
        return pl.ds(pl.multiple_of(member * rows, rows), rows)

    def head_slice(member, head):
        return pl.ds(pl.multiple_of((member * per_device + head) * HEAD, HEAD), HEAD)

    def member_device(distance):
        return (dp, flip(me, distance, members) * SEQS_CTX + core)

    def plane_device(step):
        other = (own + step) % plane
        return (other // SEQS_CTX, me * SEQS_CTX + other % SEQS_CTX)

    def copy_in(head, tensor, distance):
        if distance == 0:
            return pltpu.make_async_copy(
                sources[tensor].at[:, head_slice(me, head)],
                in_buf.at[head, tensor, row_slice(me), :],
                in_recv.at[head, tensor, 0],
            )
        return pltpu.make_async_remote_copy(
            src_ref=sources[tensor].at[:, head_slice(flip(me, distance, members), head)],
            dst_ref=in_buf.at[head, tensor, row_slice(me), :],
            send_sem=in_send.at[head, tensor, distance],
            recv_sem=in_recv.at[head, tensor, distance],
            device_id=member_device(distance),
            device_id_type=MESH,
        )

    def copy_back(head, tensor, distance):
        if distance == 0:
            return pltpu.make_async_copy(
                out_buf.at[head, tensor, row_slice(me), :],
                results[tensor].at[:, head_slice(me, head)],
                back_recv.at[head, tensor, 0],
            )
        return pltpu.make_async_remote_copy(
            src_ref=out_buf.at[head, tensor, row_slice(flip(me, distance, members)), :],
            dst_ref=results[tensor].at[:, head_slice(me, head)],
            send_sem=back_send.at[head, tensor, distance],
            recv_sem=back_recv.at[head, tensor, distance],
            device_id=member_device(distance),
            device_id_type=MESH,
        )

    def copy_places(distance):
        return pltpu.make_async_remote_copy(
            src_ref=positions,
            dst_ref=places.at[me],
            send_sem=place_send.at[distance],
            recv_sem=place_recv.at[distance],
            device_id=member_device(distance),
            device_id_type=MESH,
        )

    def copy_plane(step):
        return pltpu.make_async_remote_copy(
            src_ref=gain_part,
            dst_ref=plane_buf.at[own],
            send_sem=plane_send.at[step],
            recv_sem=plane_recv.at[step],
            device_id=plane_device(step),
            device_id_type=MESH,
        )

    def copy_group(distance):
        return pltpu.make_async_remote_copy(
            src_ref=gain_part,
            dst_ref=group_buf.at[me],
            send_sem=group_send.at[distance],
            recv_sem=group_recv.at[distance],
            device_id=member_device(distance),
            device_id_type=MESH,
        )

    barrier = pltpu.get_barrier_semaphore()
    for distance in distances:
        pl.semaphore_signal(barrier, 1, device_id=member_device(distance), device_id_type=MESH)
    for step in range(1, plane):
        pl.semaphore_signal(barrier, 1, device_id=plane_device(step), device_id_type=MESH)

    def start_own(head, carry):
        for tensor in range(4):
            copy_in(head, tensor, 0).start()
        return carry

    small_copies = [
        pltpu.make_async_copy(source, target, small_sem.at[index])
        for index, (source, target) in enumerate(
            (
                (positions, places.at[me]),
                (span_start_in, span_start),
                (span_length_in, span_length),
                (query_gain_in, query_gain),
                (key_gain_in, key_gain),
            )
        )
    ]
    for copy in small_copies:
        copy.start()
    lax.fori_loop(0, per_device, start_own, 0)
    pl.semaphore_wait(barrier, members - 1 + plane - 1)

    for distance in distances:
        copy_places(distance).start()

    def start_heads(head, carry):
        for distance in distances:
            for tensor in range(4):
                copy_in(head, tensor, distance).start()
        return carry

    lax.fori_loop(0, per_device, start_heads, 0)

    for copy in small_copies:
        copy.wait()
    for distance in distances:
        copy_places(distance).wait_recv()

    starts = [span_start[core, span] for span in range(span_start.shape[1])]
    ends = [
        starts[span] + span_length[core, span] for span in range(span_start.shape[1])
    ]

    def labels_of(place):
        label = jnp.zeros_like(place)
        for span in range(len(starts)):
            inside = (place >= starts[span]) & (place < ends[span])
            label = label + jnp.where(inside, span + 1, 0)
        return label

    def fill_bias(member, carry):
        row_places = jnp.transpose(jnp.broadcast_to(places[member], (rows, rows)))
        row_labels = labels_of(row_places)
        for other in range(members):
            key_places = jnp.broadcast_to(places[other], (rows, rows))
            key_labels = labels_of(key_places)
            allowed = (key_places <= row_places) | (
                (row_labels == key_labels) & (row_labels > 0)
            )
            bias[row_slice(member), other * rows : (other + 1) * rows] = jnp.where(
                allowed, 0.0, masked_score
            )
        return carry

    lax.fori_loop(0, members, fill_bias, 0)

    block = min(tokens, 256)

    def one_head(head, carry):
        for tensor in range(4):
            copy_in(head, tensor, 0).wait()
            for distance in distances:
                copy_in(head, tensor, distance).wait_recv()
        gain_q = query_gain[pl.ds(me * per_device + head, 1), :]
        gain_k = key_gain[pl.ds(me * per_device + head, 1), :]
        key_unit, key_inverse = unit_of(in_buf[head, 1])
        key_normed[...] = (key_unit * gain_k).astype(jnp.bfloat16)
        key_total[...] = jnp.zeros_like(key_total)
        value_total[...] = jnp.zeros_like(value_total)

        def one_block(index, query_part):
            here = pl.ds(pl.multiple_of(index * block, block), block)
            unit, inverse = unit_of(in_buf[head, 0, here, :])
            normed = (unit * gain_q).astype(jnp.bfloat16)
            values = in_buf[head, 2]
            grads = in_buf[head, 3, here, :]
            scores = dot(normed, key_normed[...], 1, 1) * scale + bias[here, :]
            row_max = jnp.max(scores, axis=-1, keepdims=True)
            powers = jnp.exp(scores - row_max)
            probs = powers * (1.0 / jnp.sum(powers, axis=-1, keepdims=True))
            weights = probs.astype(jnp.bfloat16)
            output = dot(weights, values, 1, 0).astype(jnp.bfloat16)
            out_buf[head, 0, here, :] = output
            delta = jnp.sum(
                output.astype(jnp.float32) * grads.astype(jnp.float32), axis=-1, keepdims=True
            )
            value_total[...] += dot(weights, grads, 0, 0)
            prob_grads = dot(grads, values, 1, 1)
            score_grads = (probs * (prob_grads - delta)).astype(jnp.bfloat16)
            grad_query = dot(score_grads, key_normed[...], 1, 0) * scale
            key_total[...] += dot(score_grads, normed, 0, 0)
            raw_grad, part = norm_backward(grad_query, unit, inverse, gain_q)
            out_buf[head, 1, here, :] = raw_grad
            return query_part + part

        query_part = jnp.zeros((1, HEAD), jnp.float32)
        if tokens // block <= 2:
            for index in range(tokens // block):
                query_part = one_block(index, query_part)
        else:
            query_part = lax.fori_loop(0, tokens // block, one_block, query_part)
        raw_grad, key_part = norm_backward(key_total[...] * scale, key_unit, key_inverse, gain_k)
        out_buf[head, 2] = raw_grad
        out_buf[head, 3] = value_total[...].astype(jnp.bfloat16)
        gain_part[pl.ds(head, 1), :] = query_part
        gain_part[pl.ds(per_device + head, 1), :] = key_part
        for distance in distances:
            for tensor in range(4):
                copy_back(head, tensor, distance).start()
        for tensor in range(4):
            copy_back(head, tensor, 0).start()
        return carry

    lax.fori_loop(0, per_device, one_head, 0)

    for step in range(1, plane):
        copy_plane(step).start()
    plane_buf[own] = gain_part[...]
    for step in range(1, plane):
        copy_plane(step).wait_recv()
    for step in range(1, plane):
        copy_plane(step).wait_send()
    total = plane_buf[0]
    for index in range(1, plane):
        total = total + plane_buf[index]
    gain_part[...] = total
    for distance in distances:
        copy_group(distance).start()
    group_buf[me] = total
    for distance in distances:
        copy_group(distance).wait_recv()
    for member in range(members):
        for head in range(per_device):
            at = (member * per_device + head) * HEAD
            gain_ref[0:1, at : at + HEAD] = group_buf[member, head : head + 1, :]
            gain_ref[1:2, at : at + HEAD] = group_buf[
                member, per_device + head : per_device + head + 1, :
            ]

    def finish(head, carry):
        for tensor in range(4):
            for distance in distances:
                copy_in(head, tensor, distance).wait_send()
                copy_back(head, tensor, distance).wait()
            copy_back(head, tensor, 0).wait()
        return carry

    lax.fori_loop(0, per_device, finish, 0)
    for distance in distances:
        copy_places(distance).wait_send()
        copy_group(distance).wait_send()


def place_results(*refs):
    count = len(refs) // 2
    copies = [
        pltpu.make_async_copy(refs[index], refs[count + index], refs[-1].at[index])
        for index in range(count)
    ]
    for copy in copies:
        copy.start()
    for copy in copies:
        copy.wait()


def body(
    members,
    dp_count,
    query_rows,
    key_rows,
    value_rows,
    cotangent,
    query_gain,
    key_gain,
    positions,
    span_start,
    span_length,
):
    rows, width = query_rows.shape
    heads = width // HEAD
    per_device = heads // members
    tokens = members * rows
    plane = dp_count * SEQS_CTX
    hbm = pl.BlockSpec(memory_space=pltpu.HBM)
    vmem = pl.BlockSpec(memory_space=pltpu.VMEM)
    wide = pltpu.VMEM((rows, width), jnp.bfloat16)
    dma = pltpu.SemaphoreType.DMA
    held = pl.pallas_call(
        functools.partial(kernel, members, dp_count, per_device, rows),
        out_shape=(wide, wide, wide, wide, pltpu.VMEM((2, width), jnp.float32)),
        in_specs=[hbm] * 9,
        out_specs=(vmem, vmem, vmem, vmem, vmem),
        scratch_shapes=[
            pltpu.VMEM((heads, HEAD), jnp.float32),
            pltpu.VMEM((heads, HEAD), jnp.float32),
            pltpu.SMEM(span_start.shape, jnp.int32),
            pltpu.SMEM(span_length.shape, jnp.int32),
            dma((5,)),
            pltpu.VMEM((per_device, 4, tokens, HEAD), jnp.bfloat16),
            pltpu.VMEM((per_device, 4, tokens, HEAD), jnp.bfloat16),
            pltpu.VMEM((tokens, tokens), jnp.float32),
            pltpu.VMEM((tokens, HEAD), jnp.bfloat16),
            pltpu.VMEM((tokens, HEAD), jnp.float32),
            pltpu.VMEM((tokens, HEAD), jnp.float32),
            pltpu.VMEM((members, 1, rows), jnp.int32),
            pltpu.VMEM((2 * per_device, HEAD), jnp.float32),
            pltpu.VMEM((plane, 2 * per_device, HEAD), jnp.float32),
            pltpu.VMEM((members, 2 * per_device, HEAD), jnp.float32),
            dma((per_device, 4, members)),
            dma((per_device, 4, members)),
            dma((per_device, 4, members)),
            dma((per_device, 4, members)),
            dma((members,)),
            dma((members,)),
            dma((plane,)),
            dma((plane,)),
            dma((members,)),
            dma((members,)),
        ],
        compiler_params=pltpu.CompilerParams(
            collective_id=0, has_side_effects=True, vmem_limit_bytes=123 * 512 * 1024
        ),
    )(
        query_rows,
        key_rows,
        value_rows,
        cotangent,
        query_gain.reshape(heads, HEAD),
        key_gain.reshape(heads, HEAD),
        positions.reshape(1, rows),
        span_start,
        span_length,
    )
    return pl.pallas_call(
        place_results,
        out_shape=tuple(jax.ShapeDtypeStruct(array.shape, array.dtype) for array in held),
        in_specs=[pl.BlockSpec(memory_space=pl.ANY)] * 5,
        out_specs=(pl.BlockSpec(memory_space=pltpu.HBM),) * 5,
        scratch_shapes=[dma((5,))],
        compiler_params=pltpu.CompilerParams(vmem_limit_bytes=1024 * 1024),
    )(*held)


def solution(mesh):
    row_spec = P(("dp", "ctx"), None)
    in_specs = (
        row_spec,
        row_spec,
        row_spec,
        row_spec,
        P(),
        P(),
        P(("dp", "ctx")),
        P("dp", None),
        P("dp", None),
    )
    out_specs = (row_spec, row_spec, row_spec, row_spec, P())
    members = mesh.shape["ctx"] // SEQS_CTX
    return jax.shard_map(
        functools.partial(body, members, mesh.shape["dp"]),
        mesh=mesh,
        in_specs=in_specs,
        out_specs=out_specs,
        check_vma=False,
    )
```

```python
import functools

import jax
import jax.numpy as jnp
from jax import lax
from jax.experimental import pallas as pl
from jax.experimental.pallas import tpu as pltpu
from jax.sharding import PartitionSpec as P

HEAD = 128
SEQS_CTX = 2
EARLY = 2

epsilon = 1e-05
masked_score = -1e30
MESH = pl.DeviceIdType.MESH


def flip(index, distance, count):
    result = index
    bit = 1
    while bit < count:
        if distance & bit:
            result = result + bit - 2 * bit * ((index // bit) % 2)
        bit *= 2
    return result


def unit_of(raw):
    values = raw.astype(jnp.float32)
    inverse = lax.rsqrt(jnp.mean(values * values, axis=-1, keepdims=True) + epsilon)
    return values * inverse, inverse


def norm_backward(grad_normed, unit, inverse, gain):
    grad_unit = grad_normed * gain
    projected = jnp.mean(grad_unit * unit, axis=-1, keepdims=True)
    grad_raw = inverse * (grad_unit - unit * projected)
    return grad_raw.astype(jnp.bfloat16), jnp.sum(grad_normed * unit, axis=0, keepdims=True)


def dot(left, right, left_axis, right_axis):
    return lax.dot_general(
        left,
        right,
        (((left_axis,), (right_axis,)), ((), ())),
        preferred_element_type=jnp.float32,
    )


def kernel(
    members,
    dp_count,
    per_device,
    rows,
    query_in,
    key_in,
    value_in,
    cotangent_in,
    query_gain_in,
    key_gain_in,
    positions,
    span_start_in,
    span_length_in,
    out_ref,
    query_grad_ref,
    key_grad_ref,
    value_grad_ref,
    gain_ref,
    query_gain,
    key_gain,
    span_start,
    span_length,
    small_sem,
    in_buf,
    out_buf,
    bias,
    key_normed,
    key_total,
    value_total,
    places,
    gain_part,
    plane_buf,
    group_buf,
    ready,
    in_send,
    in_recv,
    back_send,
    back_recv,
    place_send,
    place_recv,
    plane_send,
    plane_recv,
    group_send,
    group_recv,
):
    dp = lax.axis_index("dp")
    ctx = lax.axis_index("ctx")
    me = ctx // SEQS_CTX
    core = ctx % SEQS_CTX
    tokens = members * rows
    plane = dp_count * SEQS_CTX
    own = dp * SEQS_CTX + core
    sources = (query_in, key_in, value_in, cotangent_in)
    results = (out_ref, query_grad_ref, key_grad_ref, value_grad_ref)
    scale = HEAD ** (-0.5)
    half = members // 2
    upper = me // half

    def mirror(index):
        return index + upper * (members - 1 - 2 * index)

    spot = mirror(me)
    middle = (spot + 1) // half
    inner = mirror(spot + 1)
    outer = mirror(spot - 1)
    others = [mirror(members - 1 - step) for step in range(half - 1)]
    if half > 1:
        others.append(mirror(half + middle * ((spot + 1) % half - half)))
    others += [mirror((spot + step) % half) for step in range(2, half)]
    targets = others + [inner]

    def row_slice(member):
        return pl.ds(pl.multiple_of(member * rows, rows), rows)

    def head_slice(member, head):
        return pl.ds(pl.multiple_of((member * per_device + head) * HEAD, HEAD), HEAD)

    def device_of(member):
        return (dp, member * SEQS_CTX + core)

    def plane_device(bit):
        other = flip(own, bit, plane)
        return (other // SEQS_CTX, me * SEQS_CTX + other % SEQS_CTX)

    bits = [1 << index for index in range(plane.bit_length() - 1)]

    def own_in(head, tensor):
        return pltpu.make_async_copy(
            sources[tensor].at[:, head_slice(me, head)],
            in_buf.at[head, tensor, row_slice(me), :],
            in_recv.at[head, tensor, me],
        )

    def copy_in(head, tensor, target, source=me):
        return pltpu.make_async_remote_copy(
            src_ref=sources[tensor].at[:, head_slice(target, head)],
            dst_ref=in_buf.at[head, tensor, row_slice(source), :],
            send_sem=in_send.at[head, tensor, target],
            recv_sem=in_recv.at[head, tensor, source],
            device_id=device_of(target),
            device_id_type=MESH,
        )

    def own_back(head, tensor):
        return pltpu.make_async_copy(
            out_buf.at[head, tensor, row_slice(me), :],
            results[tensor].at[:, head_slice(me, head)],
            back_recv.at[head, tensor, me],
        )

    def copy_back(head, tensor, target, source=me):
        return pltpu.make_async_remote_copy(
            src_ref=out_buf.at[head, tensor, row_slice(target), :],
            dst_ref=results[tensor].at[:, head_slice(source, head)],
            send_sem=back_send.at[head, tensor, target],
            recv_sem=back_recv.at[head, tensor, source],
            device_id=device_of(target),
            device_id_type=MESH,
        )

    def copy_places(target, source=me):
        return pltpu.make_async_remote_copy(
            src_ref=positions,
            dst_ref=places.at[source],
            send_sem=place_send.at[target],
            recv_sem=place_recv.at[source],
            device_id=device_of(target),
            device_id_type=MESH,
        )

    def copy_plane(index):
        return pltpu.make_async_remote_copy(
            src_ref=gain_part.at[index],
            dst_ref=plane_buf.at[index],
            send_sem=plane_send.at[index],
            recv_sem=plane_recv.at[index],
            device_id=plane_device(bits[index]),
            device_id_type=MESH,
        )

    def copy_group(target, source=me):
        return pltpu.make_async_remote_copy(
            src_ref=gain_part.at[len(bits)],
            dst_ref=group_buf.at[source],
            send_sem=group_send.at[target],
            recv_sem=group_recv.at[source],
            device_id=device_of(target),
            device_id_type=MESH,
        )

    def signal(semaphore, device):
        pl.semaphore_signal(semaphore, 1, device_id=device, device_id_type=MESH)

    barrier = pltpu.get_barrier_semaphore()

    @pl.when(middle == 1)
    def _():
        signal(barrier, device_of(inner))

    @pl.when(spot > 0)
    def _():
        signal(barrier, device_of(outer))

    for bit in bits:
        signal(barrier, plane_device(bit))

    def start_own(head, carry):
        for tensor in range(4):
            own_in(head, tensor).start()
        return carry

    small_copies = [
        pltpu.make_async_copy(source, target, small_sem.at[index])
        for index, (source, target) in enumerate(
            (
                (positions, places.at[me]),
                (span_start_in, span_start),
                (span_length_in, span_length),
                (query_gain_in, query_gain),
                (key_gain_in, key_gain),
            )
        )
    ]
    for copy in small_copies:
        copy.start()
    lax.fori_loop(0, per_device, start_own, 0)
    pl.semaphore_wait(barrier, len(bits) + 1)

    early = min(EARLY, per_device)

    def start_inner(head, carry):
        for tensor in range(4):
            copy_in(head, tensor, inner).start()
        return carry

    copy_places(inner).start()
    lax.fori_loop(0, early, start_inner, 0)

    @pl.when(spot > 0)
    def _():
        pl.semaphore_wait(ready.at[0], 1)

    @pl.when(middle == 0)
    def _():
        signal(ready.at[0], device_of(inner))
        pl.semaphore_wait(ready.at[2], 1)

    @pl.when(middle == 1)
    def _():
        signal(ready.at[1], device_of(inner))
        pl.semaphore_wait(ready.at[1], 1)

    @pl.when(spot > 0)
    def _():
        signal(ready.at[2], device_of(outer))

    for target in others:
        copy_places(target).start()

    def start_others(head, carry):
        for target in others:
            for tensor in range(4):
                copy_in(head, tensor, target).start()
        return carry

    def start_all(head, carry):
        for target in targets:
            for tensor in range(4):
                copy_in(head, tensor, target).start()
        return carry

    lax.fori_loop(0, early, start_others, 0)
    lax.fori_loop(early, per_device, start_all, 0)

    for copy in small_copies:
        copy.wait()
    for source in targets:
        copy_places(inner, source).wait_recv()

    starts = [span_start[core, span] for span in range(span_start.shape[1])]
    ends = [
        starts[span] + span_length[core, span] for span in range(span_start.shape[1])
    ]

    def labels_of(place):
        label = jnp.zeros_like(place)
        for span in range(len(starts)):
            inside = (place >= starts[span]) & (place < ends[span])
            label = label + jnp.where(inside, span + 1, 0)
        return label

    def fill_bias(member, carry):
        row_places = jnp.transpose(jnp.broadcast_to(places[member], (rows, rows)))
        row_labels = labels_of(row_places)
        for other in range(members):
            key_places = jnp.broadcast_to(places[other], (rows, rows))
            key_labels = labels_of(key_places)
            allowed = (key_places <= row_places) | (
                (row_labels == key_labels) & (row_labels > 0)
            )
            bias[row_slice(member), other * rows : (other + 1) * rows] = jnp.where(
                allowed, 0.0, masked_score
            )
        return carry

    lax.fori_loop(0, members, fill_bias, 0)

    block = min(tokens, 256)

    def one_head(head, carry):
        for tensor in range(4):
            own_in(head, tensor).wait()
            for source in targets:
                copy_in(head, tensor, inner, source).wait_recv()
        gain_q = query_gain[pl.ds(me * per_device + head, 1), :]
        gain_k = key_gain[pl.ds(me * per_device + head, 1), :]
        key_unit, key_inverse = unit_of(in_buf[head, 1])
        key_normed[...] = (key_unit * gain_k).astype(jnp.bfloat16)
        key_total[...] = jnp.zeros_like(key_total)
        value_total[...] = jnp.zeros_like(value_total)

        def one_block(index, query_part):
            here = pl.ds(pl.multiple_of(index * block, block), block)
            unit, inverse = unit_of(in_buf[head, 0, here, :])
            normed = (unit * gain_q).astype(jnp.bfloat16)
            values = in_buf[head, 2]
            grads = in_buf[head, 3, here, :]
            scores = dot(normed, key_normed[...], 1, 1) * scale + bias[here, :]
            row_max = jnp.max(scores, axis=-1, keepdims=True)
            powers = jnp.exp(scores - row_max)
            probs = powers * (1.0 / jnp.sum(powers, axis=-1, keepdims=True))
            weights = probs.astype(jnp.bfloat16)
            output = dot(weights, values, 1, 0).astype(jnp.bfloat16)
            out_buf[head, 0, here, :] = output
            delta = jnp.sum(
                output.astype(jnp.float32) * grads.astype(jnp.float32), axis=-1, keepdims=True
            )
            value_total[...] += dot(weights, grads, 0, 0)
            prob_grads = dot(grads, values, 1, 1)
            score_grads = (probs * (prob_grads - delta)).astype(jnp.bfloat16)
            grad_query = dot(score_grads, key_normed[...], 1, 0) * scale
            key_total[...] += dot(score_grads, normed, 0, 0)
            raw_grad, part = norm_backward(grad_query, unit, inverse, gain_q)
            out_buf[head, 1, here, :] = raw_grad
            return query_part + part

        query_part = jnp.zeros((1, HEAD), jnp.float32)
        if tokens // block <= 2:
            for index in range(tokens // block):
                query_part = one_block(index, query_part)
        else:
            query_part = lax.fori_loop(0, tokens // block, one_block, query_part)
        raw_grad, key_part = norm_backward(key_total[...] * scale, key_unit, key_inverse, gain_k)
        out_buf[head, 2] = raw_grad
        out_buf[head, 3] = value_total[...].astype(jnp.bfloat16)
        gain_part[0, pl.ds(head, 1), :] = query_part
        gain_part[0, pl.ds(per_device + head, 1), :] = key_part
        for tensor in range(4):
            own_back(head, tensor).start()

        @pl.when(head < per_device - 1)
        def _():
            start_back(head)

        return carry

    def start_back(head):
        for target in targets:
            for tensor in range(4):
                copy_back(head, tensor, target).start()

    lax.fori_loop(0, per_device, one_head, 0)

    for index in range(len(bits)):
        copy_plane(index).start()
        copy_plane(index).wait_recv()
        gain_part[index + 1] = gain_part[index] + plane_buf[index]
    for target in targets:
        copy_group(target).start()
    group_buf[me] = gain_part[len(bits)]
    start_back(per_device - 1)
    for source in targets:
        copy_group(inner, source).wait_recv()
    for member in range(members):
        for head in range(per_device):
            at = (member * per_device + head) * HEAD
            gain_ref[0:1, at : at + HEAD] = group_buf[member, head : head + 1, :]
            gain_ref[1:2, at : at + HEAD] = group_buf[
                member, per_device + head : per_device + head + 1, :
            ]

    for index in range(len(bits)):
        copy_plane(index).wait_send()

    def finish(head, carry):
        for tensor in range(4):
            for member in targets:
                copy_in(head, tensor, member).wait_send()
                copy_back(head, tensor, member).wait_send()
                copy_back(head, tensor, inner, member).wait_recv()
            own_back(head, tensor).wait()
        return carry

    lax.fori_loop(0, per_device, finish, 0)
    for target in targets:
        copy_places(target).wait_send()
        copy_group(target).wait_send()


def place_results(*refs):
    count = len(refs) // 2
    copies = [
        pltpu.make_async_copy(refs[index], refs[count + index], refs[-1].at[index])
        for index in range(count)
    ]
    for copy in copies:
        copy.start()
    for copy in copies:
        copy.wait()


def body(
    members,
    dp_count,
    query_rows,
    key_rows,
    value_rows,
    cotangent,
    query_gain,
    key_gain,
    positions,
    span_start,
    span_length,
):
    rows, width = query_rows.shape
    heads = width // HEAD
    per_device = heads // members
    tokens = members * rows
    rounds = (dp_count * SEQS_CTX).bit_length() - 1
    hbm = pl.BlockSpec(memory_space=pltpu.HBM)
    vmem = pl.BlockSpec(memory_space=pltpu.VMEM)
    wide = pltpu.VMEM((rows, width), jnp.bfloat16)
    dma = pltpu.SemaphoreType.DMA
    held = pl.pallas_call(
        functools.partial(kernel, members, dp_count, per_device, rows),
        out_shape=(wide, wide, wide, wide, pltpu.VMEM((2, width), jnp.float32)),
        in_specs=[hbm] * 9,
        out_specs=(vmem, vmem, vmem, vmem, vmem),
        scratch_shapes=[
            pltpu.VMEM((heads, HEAD), jnp.float32),
            pltpu.VMEM((heads, HEAD), jnp.float32),
            pltpu.SMEM(span_start.shape, jnp.int32),
            pltpu.SMEM(span_length.shape, jnp.int32),
            dma((5,)),
            pltpu.VMEM((per_device, 4, tokens, HEAD), jnp.bfloat16),
            pltpu.VMEM((per_device, 4, tokens, HEAD), jnp.bfloat16),
            pltpu.VMEM((tokens, tokens), jnp.float32),
            pltpu.VMEM((tokens, HEAD), jnp.bfloat16),
            pltpu.VMEM((tokens, HEAD), jnp.float32),
            pltpu.VMEM((tokens, HEAD), jnp.float32),
            pltpu.VMEM((members, 1, rows), jnp.int32),
            pltpu.VMEM((rounds + 1, 2 * per_device, HEAD), jnp.float32),
            pltpu.VMEM((rounds, 2 * per_device, HEAD), jnp.float32),
            pltpu.VMEM((members, 2 * per_device, HEAD), jnp.float32),
            pltpu.SemaphoreType.REGULAR((3,)),
            dma((per_device, 4, members)),
            dma((per_device, 4, members)),
            dma((per_device, 4, members)),
            dma((per_device, 4, members)),
            dma((members,)),
            dma((members,)),
            dma((rounds,)),
            dma((rounds,)),
            dma((members,)),
            dma((members,)),
        ],
        compiler_params=pltpu.CompilerParams(
            collective_id=0, has_side_effects=True, vmem_limit_bytes=123 * 512 * 1024
        ),
    )(
        query_rows,
        key_rows,
        value_rows,
        cotangent,
        query_gain.reshape(heads, HEAD),
        key_gain.reshape(heads, HEAD),
        positions.reshape(1, rows),
        span_start,
        span_length,
    )
    return pl.pallas_call(
        place_results,
        out_shape=tuple(jax.ShapeDtypeStruct(array.shape, array.dtype) for array in held),
        in_specs=[pl.BlockSpec(memory_space=pl.ANY)] * 5,
        out_specs=(pl.BlockSpec(memory_space=pltpu.HBM),) * 5,
        scratch_shapes=[dma((5,))],
        compiler_params=pltpu.CompilerParams(vmem_limit_bytes=1024 * 1024),
    )(*held)


def solution(mesh):
    row_spec = P(("dp", "ctx"), None)
    in_specs = (
        row_spec,
        row_spec,
        row_spec,
        row_spec,
        P(),
        P(),
        P(("dp", "ctx")),
        P("dp", None),
        P("dp", None),
    )
    out_specs = (row_spec, row_spec, row_spec, row_spec, P())
    members = mesh.shape["ctx"] // SEQS_CTX
    return jax.shard_map(
        functools.partial(body, members, mesh.shape["dp"]),
        mesh=mesh,
        in_specs=in_specs,
        out_specs=out_specs,
        check_vma=False,
    )
```

```python
import functools

import jax
import jax.numpy as jnp
from jax import lax
from jax.experimental import pallas as pl
from jax.experimental.pallas import tpu as pltpu
from jax.sharding import PartitionSpec as P

HEAD = 128
SEQS_CTX = 2
EARLY = 2

epsilon = 1e-05
masked_score = -1e30
MESH = pl.DeviceIdType.MESH


def flip(index, distance, count):
    result = index
    bit = 1
    while bit < count:
        if distance & bit:
            result = result + bit - 2 * bit * ((index // bit) % 2)
        bit *= 2
    return result


def unit_of(raw):
    values = raw.astype(jnp.float32)
    inverse = lax.rsqrt(jnp.mean(values * values, axis=-1, keepdims=True) + epsilon)
    return values * inverse, inverse


def norm_backward(grad_normed, unit, inverse, gain):
    grad_unit = grad_normed * gain
    projected = jnp.mean(grad_unit * unit, axis=-1, keepdims=True)
    grad_raw = inverse * (grad_unit - unit * projected)
    return grad_raw.astype(jnp.bfloat16), jnp.sum(grad_normed * unit, axis=0, keepdims=True)


def dot(left, right, left_axis, right_axis):
    return lax.dot_general(
        left,
        right,
        (((left_axis,), (right_axis,)), ((), ())),
        preferred_element_type=jnp.float32,
    )


def kernel(
    members,
    dp_count,
    per_device,
    rows,
    query_in,
    key_in,
    value_in,
    cotangent_in,
    query_gain_in,
    key_gain_in,
    positions,
    span_start_in,
    span_length_in,
    out_ref,
    query_grad_ref,
    key_grad_ref,
    value_grad_ref,
    gain_ref,
    query_gain,
    key_gain,
    span_start,
    span_length,
    small_sem,
    in_buf,
    out_buf,
    bias,
    key_normed,
    key_total,
    value_total,
    places,
    gain_part,
    plane_buf,
    group_buf,
    ready,
    in_send,
    in_recv,
    back_send,
    back_recv,
    place_send,
    place_recv,
    plane_send,
    plane_recv,
    group_send,
    group_recv,
):
    dp = lax.axis_index("dp")
    ctx = lax.axis_index("ctx")
    me = ctx // SEQS_CTX
    core = ctx % SEQS_CTX
    tokens = members * rows
    plane = dp_count * SEQS_CTX
    own = dp * SEQS_CTX + core
    sources = (query_in, key_in, value_in, cotangent_in)
    results = (out_ref, query_grad_ref, key_grad_ref, value_grad_ref)
    scale = HEAD ** (-0.5)
    half = members // 2
    upper = me // half

    def mirror(index):
        return index + upper * (members - 1 - 2 * index)

    spot = mirror(me)
    middle = (spot + 1) // half
    inner = mirror(spot + 1)
    outer = mirror(spot - 1)
    others = [mirror(members - 1 - step) for step in range(half - 1)]
    if half > 1:
        others.append(mirror(half + middle * ((spot + 1) % half - half)))
    others += [mirror((spot + step) % half) for step in range(2, half)]
    targets = others + [inner]

    def row_slice(member):
        return pl.ds(pl.multiple_of(member * rows, rows), rows)

    def head_slice(member, head):
        return pl.ds(pl.multiple_of((member * per_device + head) * HEAD, HEAD), HEAD)

    def device_of(member):
        return (dp, member * SEQS_CTX + core)

    def plane_device(bit):
        other = flip(own, bit, plane)
        return (other // SEQS_CTX, me * SEQS_CTX + other % SEQS_CTX)

    bits = [1 << index for index in range(plane.bit_length() - 1)]

    def own_in(head, tensor):
        return pltpu.make_async_copy(
            sources[tensor].at[:, head_slice(me, head)],
            in_buf.at[head, tensor, row_slice(me), :],
            in_recv.at[head],
        )

    def copy_in(head, tensor, target):
        return pltpu.make_async_remote_copy(
            src_ref=sources[tensor].at[:, head_slice(target, head)],
            dst_ref=in_buf.at[head, tensor, row_slice(me), :],
            send_sem=in_send.at[0],
            recv_sem=in_recv.at[head],
            device_id=device_of(target),
            device_id_type=MESH,
        )

    def copy_back(head, tensor, target):
        return pltpu.make_async_remote_copy(
            src_ref=out_buf.at[head, tensor, row_slice(target), :],
            dst_ref=results[tensor].at[:, head_slice(me, head)],
            send_sem=back_send.at[0],
            recv_sem=back_recv.at[0],
            device_id=device_of(target),
            device_id_type=MESH,
        )

    def copy_places(target):
        return pltpu.make_async_remote_copy(
            src_ref=positions,
            dst_ref=places.at[me],
            send_sem=place_send.at[0],
            recv_sem=place_recv.at[0],
            device_id=device_of(target),
            device_id_type=MESH,
        )

    def copy_plane(index):
        return pltpu.make_async_remote_copy(
            src_ref=gain_part.at[index],
            dst_ref=plane_buf.at[index],
            send_sem=plane_send.at[index],
            recv_sem=plane_recv.at[index],
            device_id=plane_device(bits[index]),
            device_id_type=MESH,
        )

    def copy_group(target):
        return pltpu.make_async_remote_copy(
            src_ref=gain_part.at[len(bits)],
            dst_ref=group_buf.at[me],
            send_sem=group_send.at[0],
            recv_sem=group_recv.at[0],
            device_id=device_of(target),
            device_id_type=MESH,
        )

    def waiter(part, send, receive):
        return pltpu.make_async_remote_copy(
            src_ref=part,
            dst_ref=part,
            send_sem=send.at[0],
            recv_sem=receive,
            device_id=device_of(inner),
            device_id_type=MESH,
        )

    elsewhere = pl.ds(0, (members - 1) * rows)
    all_in = waiter(in_buf.at[:, :, elsewhere, :], in_send, in_recv.at[0])
    all_back = waiter(out_buf.at[:, :, elsewhere, :], back_send, back_recv.at[0])
    all_places = waiter(places.at[pl.ds(0, members - 1)], place_send, place_recv.at[0])
    all_group = waiter(group_buf.at[pl.ds(0, members - 1)], group_send, group_recv.at[0])

    def signal(semaphore, device):
        pl.semaphore_signal(semaphore, 1, device_id=device, device_id_type=MESH)

    barrier = pltpu.get_barrier_semaphore()

    @pl.when(middle == 1)
    def _():
        signal(barrier, device_of(inner))

    @pl.when(spot > 0)
    def _():
        signal(barrier, device_of(outer))

    @pl.when(spot == 0)
    def _():
        for bit in bits:
            signal(barrier, plane_device(bit))

    def start_own(head, carry):
        for tensor in range(4):
            own_in(head, tensor).start()
        return carry

    small_copies = [
        pltpu.make_async_copy(source, target, small_sem.at[index])
        for index, (source, target) in enumerate(
            (
                (positions, places.at[me]),
                (span_start_in, span_start),
                (span_length_in, span_length),
                (query_gain_in, query_gain),
                (key_gain_in, key_gain),
            )
        )
    ]
    for copy in small_copies:
        copy.start()
    lax.fori_loop(0, per_device, start_own, 0)
    pl.semaphore_wait(barrier, 1 + (half - spot) // half * len(bits))

    early = min(EARLY, per_device)

    def start_inner(head, carry):
        for tensor in range(4):
            copy_in(head, tensor, inner).start()
        return carry

    copy_places(inner).start()
    lax.fori_loop(0, early, start_inner, 0)

    @pl.when(spot > 0)
    def _():
        pl.semaphore_wait(ready.at[0], 1)

    @pl.when(middle == 0)
    def _():
        signal(ready.at[0], device_of(inner))
        pl.semaphore_wait(ready.at[2], 1)

    @pl.when(middle == 1)
    def _():
        signal(ready.at[1], device_of(inner))
        pl.semaphore_wait(ready.at[1], 1)

    @pl.when(spot > 0)
    def _():
        signal(ready.at[2], device_of(outer))

    @pl.when(spot == 0)
    def _():
        for bit in bits:
            signal(ready.at[3], plane_device(bit))

    for target in others:
        copy_places(target).start()

    def start_others(head, carry):
        for target in others:
            for tensor in range(4):
                copy_in(head, tensor, target).start()
        return carry

    def start_all(head, carry):
        for target in targets:
            for tensor in range(4):
                copy_in(head, tensor, target).start()
        return carry

    lax.fori_loop(0, early, start_others, 0)
    lax.fori_loop(early, per_device, start_all, 0)

    for copy in small_copies:
        copy.wait()
    all_places.wait_recv()

    starts = [span_start[core, span] for span in range(span_start.shape[1])]
    ends = [
        starts[span] + span_length[core, span] for span in range(span_start.shape[1])
    ]

    def labels_of(place):
        label = jnp.zeros_like(place)
        for span in range(len(starts)):
            inside = (place >= starts[span]) & (place < ends[span])
            label = label + jnp.where(inside, span + 1, 0)
        return label

    def fill_bias(member, carry):
        row_places = jnp.transpose(jnp.broadcast_to(places[member], (rows, rows)))
        row_labels = labels_of(row_places)
        for other in range(members):
            key_places = jnp.broadcast_to(places[other], (rows, rows))
            key_labels = labels_of(key_places)
            allowed = (key_places <= row_places) | (
                (row_labels == key_labels) & (row_labels > 0)
            )
            bias[row_slice(member), other * rows : (other + 1) * rows] = jnp.where(
                allowed, 0.0, masked_score
            )
        return carry

    lax.fori_loop(0, members, fill_bias, 0)

    block = min(tokens, 256)

    def one_head(head, carry):
        waiter(in_buf.at[head], in_send, in_recv.at[head]).wait_recv()
        gain_q = query_gain[pl.ds(me * per_device + head, 1), :]
        gain_k = key_gain[pl.ds(me * per_device + head, 1), :]
        key_unit, key_inverse = unit_of(in_buf[head, 1])
        key_normed[...] = (key_unit * gain_k).astype(jnp.bfloat16)
        key_total[...] = jnp.zeros_like(key_total)
        value_total[...] = jnp.zeros_like(value_total)

        def one_block(index, query_part):
            here = pl.ds(pl.multiple_of(index * block, block), block)
            unit, inverse = unit_of(in_buf[head, 0, here, :])
            normed = (unit * gain_q).astype(jnp.bfloat16)
            values = in_buf[head, 2]
            grads = in_buf[head, 3, here, :]
            scores = dot(normed, key_normed[...], 1, 1) * scale + bias[here, :]
            row_max = jnp.max(scores, axis=-1, keepdims=True)
            powers = jnp.exp(scores - row_max)
            probs = powers * (1.0 / jnp.sum(powers, axis=-1, keepdims=True))
            weights = probs.astype(jnp.bfloat16)
            output = dot(weights, values, 1, 0).astype(jnp.bfloat16)
            out_buf[head, 0, here, :] = output
            delta = jnp.sum(
                output.astype(jnp.float32) * grads.astype(jnp.float32), axis=-1, keepdims=True
            )
            value_total[...] += dot(weights, grads, 0, 0)
            prob_grads = dot(grads, values, 1, 1)
            score_grads = (probs * (prob_grads - delta)).astype(jnp.bfloat16)
            grad_query = dot(score_grads, key_normed[...], 1, 0) * scale
            key_total[...] += dot(score_grads, normed, 0, 0)
            raw_grad, part = norm_backward(grad_query, unit, inverse, gain_q)
            out_buf[head, 1, here, :] = raw_grad
            return query_part + part

        query_part = jnp.zeros((1, HEAD), jnp.float32)
        if tokens // block <= 2:
            for index in range(tokens // block):
                query_part = one_block(index, query_part)
        else:
            query_part = lax.fori_loop(0, tokens // block, one_block, query_part)
        raw_grad, key_part = norm_backward(key_total[...] * scale, key_unit, key_inverse, gain_k)
        out_buf[head, 2] = raw_grad
        out_buf[head, 3] = value_total[...].astype(jnp.bfloat16)
        gain_part[0, pl.ds(head, 1), :] = query_part
        gain_part[0, pl.ds(per_device + head, 1), :] = key_part
        for tensor in range(4):
            results[tensor][:, head_slice(me, head)] = out_buf[head, tensor, row_slice(me), :]

        @pl.when(head < per_device - 1)
        def _():
            start_back(head)

        return carry

    def start_back_to(head, chosen):
        for target in chosen:
            for tensor in range(4):
                copy_back(head, tensor, target).start()

    def start_back(head):
        start_back_to(head, others)

        @pl.when(head > 0)
        def _():
            start_back_to(head - 1, [inner])

    lax.fori_loop(0, per_device, one_head, 0)

    @pl.when(spot == 0)
    def _():
        pl.semaphore_wait(ready.at[3], len(bits))

    @pl.when(spot > 0)
    def _():
        pl.semaphore_wait(ready.at[4], 1)

    @pl.when(middle == 0)
    def _():
        signal(ready.at[4], device_of(inner))

    for index in range(len(bits)):
        copy_plane(index).start()
        copy_plane(index).wait_recv()
        gain_part[index + 1] = gain_part[index] + plane_buf[index]
    for target in targets:
        copy_group(target).start()
    group_buf[me] = gain_part[len(bits)]
    start_back_to(per_device - 1, others)
    if per_device > 1:
        start_back_to(per_device - 2, [inner])
    start_back_to(per_device - 1, [inner])
    all_group.wait_recv()
    for member in range(members):
        for head in range(per_device):
            at = (member * per_device + head) * HEAD
            gain_ref[0:1, at : at + HEAD] = group_buf[member, head : head + 1, :]
            gain_ref[1:2, at : at + HEAD] = group_buf[
                member, per_device + head : per_device + head + 1, :
            ]

    for index in range(len(bits)):
        copy_plane(index).wait_send()

    all_in.wait_send()
    all_places.wait_send()
    all_group.wait_send()
    all_back.wait_send()
    all_back.wait_recv()


def place_results(*refs):
    count = len(refs) // 2
    copies = [
        pltpu.make_async_copy(refs[index], refs[count + index], refs[-1].at[index])
        for index in range(count)
    ]
    for copy in copies:
        copy.start()
    for copy in copies:
        copy.wait()


def body(
    members,
    dp_count,
    query_rows,
    key_rows,
    value_rows,
    cotangent,
    query_gain,
    key_gain,
    positions,
    span_start,
    span_length,
):
    rows, width = query_rows.shape
    heads = width // HEAD
    per_device = heads // members
    tokens = members * rows
    rounds = (dp_count * SEQS_CTX).bit_length() - 1
    hbm = pl.BlockSpec(memory_space=pltpu.HBM)
    vmem = pl.BlockSpec(memory_space=pltpu.VMEM)
    wide = pltpu.VMEM((rows, width), jnp.bfloat16)
    dma = pltpu.SemaphoreType.DMA
    held = pl.pallas_call(
        functools.partial(kernel, members, dp_count, per_device, rows),
        out_shape=(wide, wide, wide, wide, pltpu.VMEM((2, width), jnp.float32)),
        in_specs=[hbm] * 9,
        out_specs=(vmem, vmem, vmem, vmem, vmem),
        scratch_shapes=[
            pltpu.VMEM((heads, HEAD), jnp.float32),
            pltpu.VMEM((heads, HEAD), jnp.float32),
            pltpu.SMEM(span_start.shape, jnp.int32),
            pltpu.SMEM(span_length.shape, jnp.int32),
            dma((5,)),
            pltpu.VMEM((per_device, 4, tokens, HEAD), jnp.bfloat16),
            pltpu.VMEM((per_device, 4, tokens, HEAD), jnp.bfloat16),
            pltpu.VMEM((tokens, tokens), jnp.float32),
            pltpu.VMEM((tokens, HEAD), jnp.bfloat16),
            pltpu.VMEM((tokens, HEAD), jnp.float32),
            pltpu.VMEM((tokens, HEAD), jnp.float32),
            pltpu.VMEM((members, 1, rows), jnp.int32),
            pltpu.VMEM((rounds + 1, 2 * per_device, HEAD), jnp.float32),
            pltpu.VMEM((rounds, 2 * per_device, HEAD), jnp.float32),
            pltpu.VMEM((members, 2 * per_device, HEAD), jnp.float32),
            pltpu.SemaphoreType.REGULAR((5,)),
            dma((1,)),
            dma((per_device,)),
            dma((1,)),
            dma((1,)),
            dma((1,)),
            dma((1,)),
            dma((rounds,)),
            dma((rounds,)),
            dma((1,)),
            dma((1,)),
        ],
        compiler_params=pltpu.CompilerParams(
            collective_id=0, has_side_effects=True, vmem_limit_bytes=123 * 512 * 1024
        ),
    )(
        query_rows,
        key_rows,
        value_rows,
        cotangent,
        query_gain.reshape(heads, HEAD),
        key_gain.reshape(heads, HEAD),
        positions.reshape(1, rows),
        span_start,
        span_length,
    )
    return pl.pallas_call(
        place_results,
        out_shape=tuple(jax.ShapeDtypeStruct(array.shape, array.dtype) for array in held),
        in_specs=[pl.BlockSpec(memory_space=pl.ANY)] * 5,
        out_specs=(pl.BlockSpec(memory_space=pltpu.HBM),) * 5,
        scratch_shapes=[dma((5,))],
        compiler_params=pltpu.CompilerParams(vmem_limit_bytes=1024 * 1024),
    )(*held)


def solution(mesh):
    row_spec = P(("dp", "ctx"), None)
    in_specs = (
        row_spec,
        row_spec,
        row_spec,
        row_spec,
        P(),
        P(),
        P(("dp", "ctx")),
        P("dp", None),
        P("dp", None),
    )
    out_specs = (row_spec, row_spec, row_spec, row_spec, P())
    members = mesh.shape["ctx"] // SEQS_CTX
    return jax.shard_map(
        functools.partial(body, members, mesh.shape["dp"]),
        mesh=mesh,
        in_specs=in_specs,
        out_specs=out_specs,
        check_vma=False,
    )
```

```python
import functools

import jax
import jax.numpy as jnp
from jax import lax
from jax.experimental import pallas as pl
from jax.experimental.pallas import tpu as pltpu
from jax.sharding import PartitionSpec as P

HEAD = 128
SEQS_CTX = 2
EARLY = 2

epsilon = 1e-05
masked_score = -1e30
MESH = pl.DeviceIdType.MESH


def flip(index, distance, count):
    result = index
    bit = 1
    while bit < count:
        if distance & bit:
            result = result + bit - 2 * bit * ((index // bit) % 2)
        bit *= 2
    return result


def unit_of(raw):
    values = raw.astype(jnp.float32)
    inverse = lax.rsqrt(jnp.mean(values * values, axis=-1, keepdims=True) + epsilon)
    return values * inverse, inverse


def norm_backward(grad_normed, unit, inverse, gain):
    grad_unit = grad_normed * gain
    projected = jnp.mean(grad_unit * unit, axis=-1, keepdims=True)
    grad_raw = inverse * (grad_unit - unit * projected)
    return grad_raw.astype(jnp.bfloat16), jnp.sum(grad_normed * unit, axis=0, keepdims=True)


def dot(left, right, left_axis, right_axis):
    return lax.dot_general(
        left,
        right,
        (((left_axis,), (right_axis,)), ((), ())),
        preferred_element_type=jnp.float32,
    )


def kernel(
    members,
    dp_count,
    per_device,
    rows,
    query_in,
    key_in,
    value_in,
    cotangent_in,
    query_gain_in,
    key_gain_in,
    positions,
    span_start_in,
    span_length_in,
    out_ref,
    query_grad_ref,
    key_grad_ref,
    value_grad_ref,
    gain_ref,
    query_gain,
    key_gain,
    span_start,
    span_length,
    small_sem,
    in_buf,
    out_buf,
    bias,
    key_normed,
    key_total,
    value_total,
    places,
    gain_part,
    plane_buf,
    group_buf,
    ready,
    in_send,
    in_recv,
    back_send,
    back_recv,
    place_send,
    place_recv,
    plane_send,
    plane_recv,
    group_send,
    group_recv,
):
    dp = lax.axis_index("dp")
    ctx = lax.axis_index("ctx")
    me = ctx // SEQS_CTX
    core = ctx % SEQS_CTX
    tokens = members * rows
    plane = dp_count * SEQS_CTX
    own = dp * SEQS_CTX + core
    sources = (query_in, key_in, value_in, cotangent_in)
    results = (out_ref, query_grad_ref, key_grad_ref, value_grad_ref)
    scale = HEAD ** (-0.5)
    half = members // 2
    upper = me // half

    def mirror(index):
        return index + upper * (members - 1 - 2 * index)

    spot = mirror(me)
    middle = (spot + 1) // half
    inner = mirror(spot + 1)
    outer = mirror(spot - 1)
    others = [mirror(members - 1 - step) for step in range(half - 1)]
    if half > 1:
        others.append(mirror(half + middle * ((spot + 1) % half - half)))
    others += [mirror((spot + step) % half) for step in range(2, half)]
    targets = others + [inner]

    def row_slice(member):
        return pl.ds(pl.multiple_of(member * rows, rows), rows)

    def head_slice(member, head):
        return pl.ds(pl.multiple_of((member * per_device + head) * HEAD, HEAD), HEAD)

    def device_of(member):
        return (dp, member * SEQS_CTX + core)

    def plane_device(bit):
        other = flip(own, bit, plane)
        return (other // SEQS_CTX, me * SEQS_CTX + other % SEQS_CTX)

    bits = [1 << index for index in range(plane.bit_length() - 1)]

    def own_in(head, tensor):
        return pltpu.make_async_copy(
            sources[tensor].at[:, head_slice(me, head)],
            in_buf.at[head, tensor, row_slice(me), :],
            in_recv.at[head],
        )

    def copy_in(head, tensor, target):
        return pltpu.make_async_remote_copy(
            src_ref=sources[tensor].at[:, head_slice(target, head)],
            dst_ref=in_buf.at[head, tensor, row_slice(me), :],
            send_sem=in_send.at[0],
            recv_sem=in_recv.at[head],
            device_id=device_of(target),
            device_id_type=MESH,
        )

    def copy_back(head, tensor, target):
        return pltpu.make_async_remote_copy(
            src_ref=out_buf.at[head, tensor, row_slice(target), :],
            dst_ref=results[tensor].at[:, head_slice(me, head)],
            send_sem=back_send.at[0],
            recv_sem=back_recv.at[0],
            device_id=device_of(target),
            device_id_type=MESH,
        )

    def copy_places(target):
        return pltpu.make_async_remote_copy(
            src_ref=positions,
            dst_ref=places.at[me],
            send_sem=place_send.at[0],
            recv_sem=place_recv.at[0],
            device_id=device_of(target),
            device_id_type=MESH,
        )

    def copy_plane(index):
        return pltpu.make_async_remote_copy(
            src_ref=gain_part.at[index],
            dst_ref=plane_buf.at[index],
            send_sem=plane_send.at[index],
            recv_sem=plane_recv.at[index],
            device_id=plane_device(bits[index]),
            device_id_type=MESH,
        )

    def copy_group(target):
        return pltpu.make_async_remote_copy(
            src_ref=gain_part.at[len(bits)],
            dst_ref=group_buf.at[me],
            send_sem=group_send.at[0],
            recv_sem=group_recv.at[0],
            device_id=device_of(target),
            device_id_type=MESH,
        )

    def waiter(part, send, receive):
        return pltpu.make_async_remote_copy(
            src_ref=part,
            dst_ref=part,
            send_sem=send.at[0],
            recv_sem=receive,
            device_id=device_of(inner),
            device_id_type=MESH,
        )

    elsewhere = pl.ds(0, (members - 1) * rows)
    all_in = waiter(in_buf.at[:, :, elsewhere, :], in_send, in_recv.at[0])
    all_back = waiter(out_buf.at[:, :, elsewhere, :], back_send, back_recv.at[0])
    all_places = waiter(places.at[pl.ds(0, members - 1)], place_send, place_recv.at[0])
    all_group = waiter(group_buf.at[pl.ds(0, members - 1)], group_send, group_recv.at[0])

    def signal(semaphore, device):
        pl.semaphore_signal(semaphore, 1, device_id=device, device_id_type=MESH)

    barrier = pltpu.get_barrier_semaphore()

    @pl.when(middle == 1)
    def _():
        signal(barrier, device_of(inner))

    @pl.when(spot > 0)
    def _():
        signal(barrier, device_of(outer))

    @pl.when(spot == 0)
    def _():
        for bit in bits:
            signal(barrier, plane_device(bit))

    pl.semaphore_wait(barrier, 1 + (half - spot) // half * len(bits))

    early = min(EARLY, per_device)

    def start_inner(head, carry):
        for tensor in range(4):
            copy_in(head, tensor, inner).start()
        return carry

    copy_places(inner).start()
    lax.fori_loop(0, early, start_inner, 0)

    def start_own(head, carry):
        for tensor in range(4):
            own_in(head, tensor).start()
        return carry

    small_copies = [
        pltpu.make_async_copy(source, target, small_sem.at[index])
        for index, (source, target) in enumerate(
            (
                (positions, places.at[me]),
                (span_start_in, span_start),
                (span_length_in, span_length),
                (query_gain_in, query_gain),
                (key_gain_in, key_gain),
            )
        )
    ]
    for copy in small_copies:
        copy.start()
    lax.fori_loop(0, per_device, start_own, 0)

    @pl.when(spot > 0)
    def _():
        pl.semaphore_wait(ready.at[0], 1)

    @pl.when(middle == 0)
    def _():
        signal(ready.at[0], device_of(inner))
        pl.semaphore_wait(ready.at[2], 1)

    @pl.when(middle == 1)
    def _():
        signal(ready.at[1], device_of(inner))
        pl.semaphore_wait(ready.at[1], 1)

    @pl.when(spot > 0)
    def _():
        signal(ready.at[2], device_of(outer))

    @pl.when(spot == 0)
    def _():
        for bit in bits:
            signal(ready.at[3], plane_device(bit))

    for target in others:
        copy_places(target).start()

    def start_others(head, carry):
        for target in others:
            for tensor in range(4):
                copy_in(head, tensor, target).start()
        return carry

    def start_all(head, carry):
        for target in targets:
            for tensor in range(4):
                copy_in(head, tensor, target).start()
        return carry

    lax.fori_loop(0, early, start_others, 0)
    lax.fori_loop(early, per_device, start_all, 0)

    for copy in small_copies:
        copy.wait()
    all_places.wait_recv()

    starts = [span_start[core, span] for span in range(span_start.shape[1])]
    ends = [
        starts[span] + span_length[core, span] for span in range(span_start.shape[1])
    ]

    def labels_of(place):
        label = jnp.zeros_like(place)
        for span in range(len(starts)):
            inside = (place >= starts[span]) & (place < ends[span])
            label = label + jnp.where(inside, span + 1, 0)
        return label

    def fill_bias(member, carry):
        row_places = jnp.transpose(jnp.broadcast_to(places[member], (rows, rows)))
        row_labels = labels_of(row_places)
        for other in range(members):
            key_places = jnp.broadcast_to(places[other], (rows, rows))
            key_labels = labels_of(key_places)
            allowed = (key_places <= row_places) | (
                (row_labels == key_labels) & (row_labels > 0)
            )
            bias[row_slice(member), other * rows : (other + 1) * rows] = jnp.where(
                allowed, 0.0, masked_score
            )
        return carry

    lax.fori_loop(0, members, fill_bias, 0)

    block = min(tokens, 256)

    def one_head(head, carry):
        waiter(in_buf.at[head], in_send, in_recv.at[head]).wait_recv()
        gain_q = query_gain[pl.ds(me * per_device + head, 1), :]
        gain_k = key_gain[pl.ds(me * per_device + head, 1), :]
        key_unit, key_inverse = unit_of(in_buf[head, 1])
        key_normed[...] = (key_unit * gain_k).astype(jnp.bfloat16)
        key_total[...] = jnp.zeros_like(key_total)
        value_total[...] = jnp.zeros_like(value_total)

        def one_block(index, query_part):
            here = pl.ds(pl.multiple_of(index * block, block), block)
            unit, inverse = unit_of(in_buf[head, 0, here, :])
            normed = (unit * gain_q).astype(jnp.bfloat16)
            values = in_buf[head, 2]
            grads = in_buf[head, 3, here, :]
            scores = dot(normed, key_normed[...], 1, 1) * scale + bias[here, :]
            row_max = jnp.max(scores, axis=-1, keepdims=True)
            powers = jnp.exp(scores - row_max)
            probs = powers * (1.0 / jnp.sum(powers, axis=-1, keepdims=True))
            weights = probs.astype(jnp.bfloat16)
            output = dot(weights, values, 1, 0).astype(jnp.bfloat16)
            out_buf[head, 0, here, :] = output
            delta = jnp.sum(
                output.astype(jnp.float32) * grads.astype(jnp.float32), axis=-1, keepdims=True
            )
            value_total[...] += dot(weights, grads, 0, 0)
            prob_grads = dot(grads, values, 1, 1)
            score_grads = (probs * (prob_grads - delta)).astype(jnp.bfloat16)
            grad_query = dot(score_grads, key_normed[...], 1, 0) * scale
            key_total[...] += dot(score_grads, normed, 0, 0)
            raw_grad, part = norm_backward(grad_query, unit, inverse, gain_q)
            out_buf[head, 1, here, :] = raw_grad
            return query_part + part

        query_part = jnp.zeros((1, HEAD), jnp.float32)
        if tokens // block <= 2:
            for index in range(tokens // block):
                query_part = one_block(index, query_part)
        else:
            query_part = lax.fori_loop(0, tokens // block, one_block, query_part)
        raw_grad, key_part = norm_backward(key_total[...] * scale, key_unit, key_inverse, gain_k)
        out_buf[head, 2] = raw_grad
        out_buf[head, 3] = value_total[...].astype(jnp.bfloat16)
        gain_part[0, pl.ds(head, 1), :] = query_part
        gain_part[0, pl.ds(per_device + head, 1), :] = key_part
        for tensor in range(4):
            results[tensor][:, head_slice(me, head)] = out_buf[head, tensor, row_slice(me), :]

        @pl.when(head < per_device - 1)
        def _():
            start_back(head)

        return carry

    def start_back_to(head, chosen):
        for target in chosen:
            for tensor in range(4):
                copy_back(head, tensor, target).start()

    def start_back(head):
        start_back_to(head, others)

        @pl.when(head > 0)
        def _():
            start_back_to(head - 1, [inner])

    lax.fori_loop(0, per_device, one_head, 0)
    start_back_to(per_device - 1, others)

    @pl.when(spot == 0)
    def _():
        pl.semaphore_wait(ready.at[3], len(bits))

    @pl.when(spot > 0)
    def _():
        pl.semaphore_wait(ready.at[4], 1)

    @pl.when(middle == 0)
    def _():
        signal(ready.at[4], device_of(inner))

    for index in range(len(bits)):
        copy_plane(index).start()
        copy_plane(index).wait_recv()
        gain_part[index + 1] = gain_part[index] + plane_buf[index]
    for target in targets:
        copy_group(target).start()
    group_buf[me] = gain_part[len(bits)]
    if per_device > 1:
        start_back_to(per_device - 2, [inner])
    start_back_to(per_device - 1, [inner])
    all_group.wait_recv()
    for member in range(members):
        for head in range(per_device):
            at = (member * per_device + head) * HEAD
            gain_ref[0:1, at : at + HEAD] = group_buf[member, head : head + 1, :]
            gain_ref[1:2, at : at + HEAD] = group_buf[
                member, per_device + head : per_device + head + 1, :
            ]

    for index in range(len(bits)):
        copy_plane(index).wait_send()

    all_in.wait_send()
    all_places.wait_send()
    all_group.wait_send()
    all_back.wait_send()
    all_back.wait_recv()


def place_results(*refs):
    count = len(refs) // 2
    copies = [
        pltpu.make_async_copy(refs[index], refs[count + index], refs[-1].at[index])
        for index in range(count)
    ]
    for copy in copies:
        copy.start()
    for copy in copies:
        copy.wait()


def body(
    members,
    dp_count,
    query_rows,
    key_rows,
    value_rows,
    cotangent,
    query_gain,
    key_gain,
    positions,
    span_start,
    span_length,
):
    rows, width = query_rows.shape
    heads = width // HEAD
    per_device = heads // members
    tokens = members * rows
    rounds = (dp_count * SEQS_CTX).bit_length() - 1
    hbm = pl.BlockSpec(memory_space=pltpu.HBM)
    vmem = pl.BlockSpec(memory_space=pltpu.VMEM)
    wide = pltpu.VMEM((rows, width), jnp.bfloat16)
    dma = pltpu.SemaphoreType.DMA
    held = pl.pallas_call(
        functools.partial(kernel, members, dp_count, per_device, rows),
        out_shape=(wide, wide, wide, wide, pltpu.VMEM((2, width), jnp.float32)),
        in_specs=[hbm] * 9,
        out_specs=(vmem, vmem, vmem, vmem, vmem),
        scratch_shapes=[
            pltpu.VMEM((heads, HEAD), jnp.float32),
            pltpu.VMEM((heads, HEAD), jnp.float32),
            pltpu.SMEM(span_start.shape, jnp.int32),
            pltpu.SMEM(span_length.shape, jnp.int32),
            dma((5,)),
            pltpu.VMEM((per_device, 4, tokens, HEAD), jnp.bfloat16),
            pltpu.VMEM((per_device, 4, tokens, HEAD), jnp.bfloat16),
            pltpu.VMEM((tokens, tokens), jnp.float32),
            pltpu.VMEM((tokens, HEAD), jnp.bfloat16),
            pltpu.VMEM((tokens, HEAD), jnp.float32),
            pltpu.VMEM((tokens, HEAD), jnp.float32),
            pltpu.VMEM((members, 1, rows), jnp.int32),
            pltpu.VMEM((rounds + 1, 2 * per_device, HEAD), jnp.float32),
            pltpu.VMEM((rounds, 2 * per_device, HEAD), jnp.float32),
            pltpu.VMEM((members, 2 * per_device, HEAD), jnp.float32),
            pltpu.SemaphoreType.REGULAR((5,)),
            dma((1,)),
            dma((per_device,)),
            dma((1,)),
            dma((1,)),
            dma((1,)),
            dma((1,)),
            dma((rounds,)),
            dma((rounds,)),
            dma((1,)),
            dma((1,)),
        ],
        compiler_params=pltpu.CompilerParams(
            collective_id=0, has_side_effects=True, vmem_limit_bytes=123 * 512 * 1024
        ),
    )(
        query_rows,
        key_rows,
        value_rows,
        cotangent,
        query_gain.reshape(heads, HEAD),
        key_gain.reshape(heads, HEAD),
        positions.reshape(1, rows),
        span_start,
        span_length,
    )
    return pl.pallas_call(
        place_results,
        out_shape=tuple(jax.ShapeDtypeStruct(array.shape, array.dtype) for array in held),
        in_specs=[pl.BlockSpec(memory_space=pl.ANY)] * 5,
        out_specs=(pl.BlockSpec(memory_space=pltpu.HBM),) * 5,
        scratch_shapes=[dma((5,))],
        compiler_params=pltpu.CompilerParams(vmem_limit_bytes=1024 * 1024),
    )(*held)


def solution(mesh):
    row_spec = P(("dp", "ctx"), None)
    in_specs = (
        row_spec,
        row_spec,
        row_spec,
        row_spec,
        P(),
        P(),
        P(("dp", "ctx")),
        P("dp", None),
        P("dp", None),
    )
    out_specs = (row_spec, row_spec, row_spec, row_spec, P())
    members = mesh.shape["ctx"] // SEQS_CTX
    return jax.shard_map(
        functools.partial(body, members, mesh.shape["dp"]),
        mesh=mesh,
        in_specs=in_specs,
        out_specs=out_specs,
        check_vma=False,
    )
```

```python
import functools

import jax
import jax.numpy as jnp
from jax import lax
from jax.experimental import pallas as pl
from jax.experimental.pallas import tpu as pltpu
from jax.sharding import PartitionSpec as P

HEAD = 128
SEQS_CTX = 2
EARLY = 2
RELAYED = 1

epsilon = 1e-05
masked_score = -1e30
MESH = pl.DeviceIdType.MESH


def flip(index, distance, count):
    result = index
    bit = 1
    while bit < count:
        if distance & bit:
            result = result + bit - 2 * bit * ((index // bit) % 2)
        bit *= 2
    return result


def unit_of(raw):
    values = raw.astype(jnp.float32)
    inverse = lax.rsqrt(jnp.mean(values * values, axis=-1, keepdims=True) + epsilon)
    return values * inverse, inverse


def norm_backward(grad_normed, unit, inverse, gain):
    grad_unit = grad_normed * gain
    projected = jnp.mean(grad_unit * unit, axis=-1, keepdims=True)
    grad_raw = inverse * (grad_unit - unit * projected)
    return grad_raw.astype(jnp.bfloat16), jnp.sum(grad_normed * unit, axis=0, keepdims=True)


def dot(left, right, left_axis, right_axis):
    return lax.dot_general(
        left,
        right,
        (((left_axis,), (right_axis,)), ((), ())),
        preferred_element_type=jnp.float32,
    )


def kernel(
    members,
    dp_count,
    per_device,
    rows,
    query_in,
    key_in,
    value_in,
    cotangent_in,
    query_gain_in,
    key_gain_in,
    positions,
    span_start_in,
    span_length_in,
    out_ref,
    query_grad_ref,
    key_grad_ref,
    value_grad_ref,
    gain_ref,
    query_gain,
    key_gain,
    span_start,
    span_length,
    small_sem,
    in_buf,
    out_buf,
    bias,
    key_normed,
    key_total,
    value_total,
    places,
    gain_part,
    plane_buf,
    group_buf,
    relay_buf,
    ready,
    in_send,
    in_recv,
    back_send,
    back_recv,
    place_send,
    place_recv,
    plane_send,
    plane_recv,
    group_send,
    group_recv,
    share_send,
    share_recv,
    relay_send,
    relay_recv,
):
    dp = lax.axis_index("dp")
    ctx = lax.axis_index("ctx")
    me = ctx // SEQS_CTX
    core = ctx % SEQS_CTX
    tokens = members * rows
    plane = dp_count * SEQS_CTX
    own = dp * SEQS_CTX + core
    sources = (query_in, key_in, value_in, cotangent_in)
    results = (out_ref, query_grad_ref, key_grad_ref, value_grad_ref)
    scale = HEAD ** (-0.5)
    half = members // 2
    upper = me // half

    def mirror(index):
        return index + upper * (members - 1 - 2 * index)

    spot = mirror(me)
    middle = (spot + 1) // half
    inner = mirror(spot + 1)
    outer = mirror(spot - 1)
    others = [mirror(members - 1 - step) for step in range(half - 1)]
    if half > 1:
        others.append(mirror(half + middle * ((spot + 1) % half - half)))
    others += [mirror((spot + step) % half) for step in range(2, half)]
    targets = others + [inner]

    def row_slice(member):
        return pl.ds(pl.multiple_of(member * rows, rows), rows)

    def head_slice(member, head):
        return pl.ds(pl.multiple_of((member * per_device + head) * HEAD, HEAD), HEAD)

    def device_of(member):
        return (dp, member * SEQS_CTX + core)

    def plane_device(bit):
        other = flip(own, bit, plane)
        return (other // SEQS_CTX, me * SEQS_CTX + other % SEQS_CTX)

    bits = [1 << index for index in range(plane.bit_length() - 1)]

    def own_in(head, tensor):
        return pltpu.make_async_copy(
            sources[tensor].at[:, head_slice(me, head)],
            in_buf.at[head, tensor, row_slice(me), :],
            in_recv.at[head],
        )

    def copy_in(head, tensor, target):
        return pltpu.make_async_remote_copy(
            src_ref=sources[tensor].at[:, head_slice(target, head)],
            dst_ref=in_buf.at[head, tensor, row_slice(me), :],
            send_sem=in_send.at[0],
            recv_sem=in_recv.at[head],
            device_id=device_of(target),
            device_id_type=MESH,
        )

    def copy_back(head, tensor, target):
        return pltpu.make_async_remote_copy(
            src_ref=out_buf.at[head, tensor, row_slice(target), :],
            dst_ref=results[tensor].at[:, head_slice(me, head)],
            send_sem=back_send.at[0],
            recv_sem=back_recv.at[0],
            device_id=device_of(target),
            device_id_type=MESH,
        )

    carried = range(4 - (RELAYED if per_device > 1 else 0), 4)
    gives = middle * (1 - core)
    carries = middle * core
    first_of = lambda index: 1 - jnp.minimum(index, 1)
    other_core = (dp, me * SEQS_CTX + 1 - core)

    def copy_over(tensor):
        return pltpu.make_async_remote_copy(
            src_ref=out_buf.at[0, tensor, row_slice(inner), :],
            dst_ref=relay_buf.at[tensor - carried[0]],
            send_sem=back_send.at[0],
            recv_sem=relay_recv.at[0],
            device_id=other_core,
            device_id_type=MESH,
        )

    def copy_carried(tensor):
        return pltpu.make_async_remote_copy(
            src_ref=relay_buf.at[tensor - carried[0]],
            dst_ref=results[tensor].at[:, head_slice(me, 0)],
            send_sem=relay_send.at[0],
            recv_sem=back_recv.at[0],
            device_id=(dp, inner * SEQS_CTX),
            device_id_type=MESH,
        )

    def copy_share():
        return pltpu.make_async_remote_copy(
            src_ref=group_buf,
            dst_ref=group_buf,
            send_sem=share_send.at[0],
            recv_sem=share_recv.at[0],
            device_id=other_core,
            device_id_type=MESH,
        )

    def copy_places(target):
        return pltpu.make_async_remote_copy(
            src_ref=positions,
            dst_ref=places.at[me],
            send_sem=place_send.at[0],
            recv_sem=place_recv.at[0],
            device_id=device_of(target),
            device_id_type=MESH,
        )

    def copy_plane(index):
        return pltpu.make_async_remote_copy(
            src_ref=gain_part.at[index],
            dst_ref=plane_buf.at[index],
            send_sem=plane_send.at[index],
            recv_sem=plane_recv.at[index],
            device_id=plane_device(bits[index]),
            device_id_type=MESH,
        )

    def copy_group(target):
        return pltpu.make_async_remote_copy(
            src_ref=gain_part.at[len(bits)],
            dst_ref=group_buf.at[me],
            send_sem=group_send.at[0],
            recv_sem=group_recv.at[0],
            device_id=device_of(target),
            device_id_type=MESH,
        )

    def waiter(part, send, receive):
        return pltpu.make_async_remote_copy(
            src_ref=part,
            dst_ref=part,
            send_sem=send.at[0],
            recv_sem=receive,
            device_id=device_of(inner),
            device_id_type=MESH,
        )

    elsewhere = pl.ds(0, (members - 1) * rows)
    all_in = waiter(in_buf.at[:, :, elsewhere, :], in_send, in_recv.at[0])
    all_back = waiter(out_buf.at[:, :, elsewhere, :], back_send, back_recv.at[0])
    all_places = waiter(places.at[pl.ds(0, members - 1)], place_send, place_recv.at[0])
    all_group = waiter(group_buf.at[pl.ds(0, members - 1)], group_send, group_recv.at[0])

    def signal(semaphore, device):
        pl.semaphore_signal(semaphore, 1, device_id=device, device_id_type=MESH)

    barrier = pltpu.get_barrier_semaphore()

    @pl.when(middle == 1)
    def _():
        signal(barrier, device_of(inner))

    @pl.when(spot > 0)
    def _():
        signal(barrier, device_of(outer))

    @pl.when(spot == 0)
    def _():
        for bit in bits:
            signal(barrier, plane_device(bit))

    pl.semaphore_wait(barrier, 1 + (half - spot) // half * len(bits))

    early = min(EARLY, per_device)

    def start_inner(head, carry):
        for tensor in range(4):
            copy_in(head, tensor, inner).start()
        return carry

    copy_places(inner).start()
    lax.fori_loop(0, early, start_inner, 0)

    def start_own(head, carry):
        for tensor in range(4):
            own_in(head, tensor).start()
        return carry

    small_copies = [
        pltpu.make_async_copy(source, target, small_sem.at[index])
        for index, (source, target) in enumerate(
            (
                (positions, places.at[me]),
                (span_start_in, span_start),
                (span_length_in, span_length),
                (query_gain_in, query_gain),
                (key_gain_in, key_gain),
            )
        )
    ]
    for copy in small_copies:
        copy.start()
    lax.fori_loop(0, per_device, start_own, 0)

    @pl.when(spot > 0)
    def _():
        pl.semaphore_wait(ready.at[0], 1)

    @pl.when(middle == 0)
    def _():
        signal(ready.at[0], device_of(inner))
        pl.semaphore_wait(ready.at[2], 1)

    @pl.when(middle == 1)
    def _():
        signal(ready.at[1], device_of(inner))
        pl.semaphore_wait(ready.at[1], 1)

    @pl.when(spot > 0)
    def _():
        signal(ready.at[2], device_of(outer))

    @pl.when(spot == 0)
    def _():
        for bit in bits:
            signal(ready.at[3], plane_device(bit))

    for target in others:
        copy_places(target).start()

    def start_others(head, carry):
        for target in others:
            for tensor in range(4):
                copy_in(head, tensor, target).start()
        return carry

    def start_all(head, carry):
        for target in targets:
            for tensor in range(4):
                copy_in(head, tensor, target).start()
        return carry

    lax.fori_loop(0, early, start_others, 0)
    lax.fori_loop(early, per_device, start_all, 0)

    for copy in small_copies:
        copy.wait()
    all_places.wait_recv()

    starts = [span_start[core, span] for span in range(span_start.shape[1])]
    ends = [
        starts[span] + span_length[core, span] for span in range(span_start.shape[1])
    ]

    def labels_of(place):
        label = jnp.zeros_like(place)
        for span in range(len(starts)):
            inside = (place >= starts[span]) & (place < ends[span])
            label = label + jnp.where(inside, span + 1, 0)
        return label

    def fill_bias(member, carry):
        row_places = jnp.transpose(jnp.broadcast_to(places[member], (rows, rows)))
        row_labels = labels_of(row_places)
        for other in range(members):
            key_places = jnp.broadcast_to(places[other], (rows, rows))
            key_labels = labels_of(key_places)
            allowed = (key_places <= row_places) | (
                (row_labels == key_labels) & (row_labels > 0)
            )
            bias[row_slice(member), other * rows : (other + 1) * rows] = jnp.where(
                allowed, 0.0, masked_score
            )
        return carry

    lax.fori_loop(0, members, fill_bias, 0)

    block = min(tokens, 256)

    def one_head(head, carry):
        waiter(in_buf.at[head], in_send, in_recv.at[head]).wait_recv()
        gain_q = query_gain[pl.ds(me * per_device + head, 1), :]
        gain_k = key_gain[pl.ds(me * per_device + head, 1), :]
        key_unit, key_inverse = unit_of(in_buf[head, 1])
        key_normed[...] = (key_unit * gain_k).astype(jnp.bfloat16)
        key_total[...] = jnp.zeros_like(key_total)
        value_total[...] = jnp.zeros_like(value_total)

        def one_block(index, query_part):
            here = pl.ds(pl.multiple_of(index * block, block), block)
            unit, inverse = unit_of(in_buf[head, 0, here, :])
            normed = (unit * gain_q).astype(jnp.bfloat16)
            values = in_buf[head, 2]
            grads = in_buf[head, 3, here, :]
            scores = dot(normed, key_normed[...], 1, 1) * scale + bias[here, :]
            row_max = jnp.max(scores, axis=-1, keepdims=True)
            powers = jnp.exp(scores - row_max)
            probs = powers * (1.0 / jnp.sum(powers, axis=-1, keepdims=True))
            weights = probs.astype(jnp.bfloat16)
            output = dot(weights, values, 1, 0).astype(jnp.bfloat16)
            out_buf[head, 0, here, :] = output
            delta = jnp.sum(
                output.astype(jnp.float32) * grads.astype(jnp.float32), axis=-1, keepdims=True
            )
            value_total[...] += dot(weights, grads, 0, 0)
            prob_grads = dot(grads, values, 1, 1)
            score_grads = (probs * (prob_grads - delta)).astype(jnp.bfloat16)
            grad_query = dot(score_grads, key_normed[...], 1, 0) * scale
            key_total[...] += dot(score_grads, normed, 0, 0)
            raw_grad, part = norm_backward(grad_query, unit, inverse, gain_q)
            out_buf[head, 1, here, :] = raw_grad
            return query_part + part

        query_part = jnp.zeros((1, HEAD), jnp.float32)
        if tokens // block <= 2:
            for index in range(tokens // block):
                query_part = one_block(index, query_part)
        else:
            query_part = lax.fori_loop(0, tokens // block, one_block, query_part)
        raw_grad, key_part = norm_backward(key_total[...] * scale, key_unit, key_inverse, gain_k)
        out_buf[head, 2] = raw_grad
        out_buf[head, 3] = value_total[...].astype(jnp.bfloat16)
        gain_part[0, pl.ds(head, 1), :] = query_part
        gain_part[0, pl.ds(per_device + head, 1), :] = key_part
        for tensor in range(4):
            results[tensor][:, head_slice(me, head)] = out_buf[head, tensor, row_slice(me), :]

        if len(carried) > 0:

            @pl.when(gives * first_of(head) == 1)
            def _():
                for tensor in carried:
                    copy_over(tensor).start()

            @pl.when(carries * first_of(jnp.abs(head - 1)) == 1)
            def _():
                waiter(relay_buf, relay_send, relay_recv.at[0]).wait_recv()
                for tensor in carried:
                    copy_carried(tensor).start()

        @pl.when(head < per_device - 1)
        def _():
            start_back(head)

        return carry

    def start_back_to(head, chosen, tensors=range(4)):
        for target in chosen:
            for tensor in tensors:
                copy_back(head, tensor, target).start()

    def start_back_inner(head):
        start_back_to(head, [inner], range(carried[0] if len(carried) > 0 else 4))
        if len(carried) > 0:

            @pl.when(gives * first_of(head) == 0)
            def _():
                start_back_to(head, [inner], carried)

    def start_back(head):
        start_back_to(head, others)

        @pl.when(head > 0)
        def _():
            start_back_inner(head - 1)

    @pl.when(spot == 0)
    def _():
        pl.semaphore_wait(ready.at[3], len(bits))

    @pl.when(spot > 0)
    def _():
        pl.semaphore_wait(ready.at[4], 1)

    @pl.when(middle == 0)
    def _():
        signal(ready.at[4], device_of(inner))

    lax.fori_loop(0, per_device, one_head, 0)
    start_back_to(per_device - 1, others)

    for index in range(len(bits)):
        copy_plane(index).start()
        copy_plane(index).wait_recv()
        gain_part[index + 1] = gain_part[index] + plane_buf[index]
    @pl.when(core == 1)
    def _():
        group_buf[me] = gain_part[len(bits)]
        for target in targets:
            copy_group(target).start()

    if per_device > 1:
        start_back_inner(per_device - 2)
    start_back_inner(per_device - 1)

    @pl.when(core == 1)
    def _():
        all_group.wait_recv()
        copy_share().start()

    @pl.when(core == 0)
    def _():
        copy_share().wait_recv()

    for member in range(members):
        for head in range(per_device):
            at = (member * per_device + head) * HEAD
            gain_ref[0:1, at : at + HEAD] = group_buf[member, head : head + 1, :]
            gain_ref[1:2, at : at + HEAD] = group_buf[
                member, per_device + head : per_device + head + 1, :
            ]

    for index in range(len(bits)):
        copy_plane(index).wait_send()

    all_in.wait_send()
    all_places.wait_send()

    @pl.when(core == 1)
    def _():
        all_group.wait_send()
        copy_share().wait_send()

    all_back.wait_send()
    if len(carried) > 0:

        @pl.when(carries == 1)
        def _():
            waiter(relay_buf, relay_send, relay_recv.at[0]).wait_send()

    all_back.wait_recv()


def place_results(*refs):
    count = len(refs) // 2
    copies = [
        pltpu.make_async_copy(refs[index], refs[count + index], refs[-1].at[index])
        for index in range(count)
    ]
    for copy in copies:
        copy.start()
    for copy in copies:
        copy.wait()


def body(
    members,
    dp_count,
    query_rows,
    key_rows,
    value_rows,
    cotangent,
    query_gain,
    key_gain,
    positions,
    span_start,
    span_length,
):
    rows, width = query_rows.shape
    heads = width // HEAD
    per_device = heads // members
    tokens = members * rows
    rounds = (dp_count * SEQS_CTX).bit_length() - 1
    hbm = pl.BlockSpec(memory_space=pltpu.HBM)
    vmem = pl.BlockSpec(memory_space=pltpu.VMEM)
    wide = pltpu.VMEM((rows, width), jnp.bfloat16)
    dma = pltpu.SemaphoreType.DMA
    held = pl.pallas_call(
        functools.partial(kernel, members, dp_count, per_device, rows),
        out_shape=(wide, wide, wide, wide, pltpu.VMEM((2, width), jnp.float32)),
        in_specs=[hbm] * 9,
        out_specs=(vmem, vmem, vmem, vmem, vmem),
        scratch_shapes=[
            pltpu.VMEM((heads, HEAD), jnp.float32),
            pltpu.VMEM((heads, HEAD), jnp.float32),
            pltpu.SMEM(span_start.shape, jnp.int32),
            pltpu.SMEM(span_length.shape, jnp.int32),
            dma((5,)),
            pltpu.VMEM((per_device, 4, tokens, HEAD), jnp.bfloat16),
            pltpu.VMEM((per_device, 4, tokens, HEAD), jnp.bfloat16),
            pltpu.VMEM((tokens, tokens), jnp.float32),
            pltpu.VMEM((tokens, HEAD), jnp.bfloat16),
            pltpu.VMEM((tokens, HEAD), jnp.float32),
            pltpu.VMEM((tokens, HEAD), jnp.float32),
            pltpu.VMEM((members, 1, rows), jnp.int32),
            pltpu.VMEM((rounds + 1, 2 * per_device, HEAD), jnp.float32),
            pltpu.VMEM((rounds, 2 * per_device, HEAD), jnp.float32),
            pltpu.VMEM((members, 2 * per_device, HEAD), jnp.float32),
            pltpu.VMEM((max(RELAYED, 1), rows, HEAD), jnp.bfloat16),
            pltpu.SemaphoreType.REGULAR((5,)),
            dma((1,)),
            dma((per_device,)),
            dma((1,)),
            dma((1,)),
            dma((1,)),
            dma((1,)),
            dma((rounds,)),
            dma((rounds,)),
            dma((1,)),
            dma((1,)),
            dma((1,)),
            dma((1,)),
            dma((1,)),
            dma((1,)),
        ],
        compiler_params=pltpu.CompilerParams(
            collective_id=0, has_side_effects=True, vmem_limit_bytes=123 * 512 * 1024
        ),
    )(
        query_rows,
        key_rows,
        value_rows,
        cotangent,
        query_gain.reshape(heads, HEAD),
        key_gain.reshape(heads, HEAD),
        positions.reshape(1, rows),
        span_start,
        span_length,
    )
    return pl.pallas_call(
        place_results,
        out_shape=tuple(jax.ShapeDtypeStruct(array.shape, array.dtype) for array in held),
        in_specs=[pl.BlockSpec(memory_space=pl.ANY)] * 5,
        out_specs=(pl.BlockSpec(memory_space=pltpu.HBM),) * 5,
        scratch_shapes=[dma((5,))],
        compiler_params=pltpu.CompilerParams(vmem_limit_bytes=1024 * 1024),
    )(*held)


def solution(mesh):
    row_spec = P(("dp", "ctx"), None)
    in_specs = (
        row_spec,
        row_spec,
        row_spec,
        row_spec,
        P(),
        P(),
        P(("dp", "ctx")),
        P("dp", None),
        P("dp", None),
    )
    out_specs = (row_spec, row_spec, row_spec, row_spec, P())
    members = mesh.shape["ctx"] // SEQS_CTX
    return jax.shard_map(
        functools.partial(body, members, mesh.shape["dp"]),
        mesh=mesh,
        in_specs=in_specs,
        out_specs=out_specs,
        check_vma=False,
    )
```

```python
import functools

import jax
import jax.numpy as jnp
from jax import lax
from jax.experimental import pallas as pl
from jax.experimental.pallas import tpu as pltpu
from jax.sharding import PartitionSpec as P

HEAD = 128
SEQS_CTX = 2
EARLY = 2

epsilon = 1e-05
masked_score = -1e30
MESH = pl.DeviceIdType.MESH


def flip(index, distance, count):
    result = index
    bit = 1
    while bit < count:
        if distance & bit:
            result = result + bit - 2 * bit * ((index // bit) % 2)
        bit *= 2
    return result


def unit_of(raw):
    values = raw.astype(jnp.float32)
    inverse = lax.rsqrt(jnp.mean(values * values, axis=-1, keepdims=True) + epsilon)
    return values * inverse, inverse


def norm_backward(grad_normed, unit, inverse, gain):
    grad_unit = grad_normed * gain
    projected = jnp.mean(grad_unit * unit, axis=-1, keepdims=True)
    grad_raw = inverse * (grad_unit - unit * projected)
    return grad_raw.astype(jnp.bfloat16), jnp.sum(grad_normed * unit, axis=0, keepdims=True)


def dot(left, right, left_axis, right_axis):
    return lax.dot_general(
        left,
        right,
        (((left_axis,), (right_axis,)), ((), ())),
        preferred_element_type=jnp.float32,
    )


def kernel(
    members,
    dp_count,
    per_device,
    rows,
    query_in,
    key_in,
    value_in,
    cotangent_in,
    query_gain_in,
    key_gain_in,
    positions,
    span_start_in,
    span_length_in,
    out_ref,
    query_grad_ref,
    key_grad_ref,
    value_grad_ref,
    gain_ref,
    gains,
    spans,
    small_sem,
    in_buf,
    out_buf,
    bias,
    key_normed,
    key_total,
    value_total,
    places,
    gain_part,
    plane_buf,
    group_buf,
    ready,
    in_send,
    in_recv,
    back_send,
    back_recv,
    place_send,
    place_recv,
    plane_send,
    plane_recv,
    group_send,
    group_recv,
    share_send,
    share_recv,
):
    dp = lax.axis_index("dp")
    ctx = lax.axis_index("ctx")
    me = ctx // SEQS_CTX
    core = ctx % SEQS_CTX
    tokens = members * rows
    plane = dp_count * SEQS_CTX
    own = dp * SEQS_CTX + core
    sources = (query_in, key_in, value_in, cotangent_in)
    results = (out_ref, query_grad_ref, key_grad_ref, value_grad_ref)
    scale = HEAD ** (-0.5)
    half = members // 2
    upper = me // half

    def mirror(index):
        return index + upper * (members - 1 - 2 * index)

    spot = mirror(me)
    middle = (spot + 1) // half
    inner = mirror(spot + 1)
    outer = mirror(spot - 1)
    others = [mirror(members - 1 - step) for step in range(half - 1)]
    if half > 1:
        others.append(mirror(half + middle * ((spot + 1) % half - half)))
    others += [mirror((spot + step) % half) for step in range(2, half)]
    targets = others + [inner]

    def row_slice(member):
        return pl.ds(pl.multiple_of(member * rows, rows), rows)

    def head_slice(member, head):
        return pl.ds(pl.multiple_of((member * per_device + head) * HEAD, HEAD), HEAD)

    def device_of(member):
        return (dp, member * SEQS_CTX + core)

    def plane_device(bit):
        other = flip(own, bit, plane)
        return (other // SEQS_CTX, me * SEQS_CTX + other % SEQS_CTX)

    bits = [1 << index for index in range(plane.bit_length() - 1)]

    def own_in(head, tensor):
        return pltpu.make_async_copy(
            sources[tensor].at[:, head_slice(me, head)],
            in_buf.at[head, tensor, row_slice(me), :],
            in_recv.at[head],
        )

    def copy_in(head, tensor, target):
        return pltpu.make_async_remote_copy(
            src_ref=sources[tensor].at[:, head_slice(target, head)],
            dst_ref=in_buf.at[head, tensor, row_slice(me), :],
            send_sem=in_send.at[0],
            recv_sem=in_recv.at[head],
            device_id=device_of(target),
            device_id_type=MESH,
        )

    def copy_back(head, tensor, target):
        return pltpu.make_async_remote_copy(
            src_ref=out_buf.at[head, tensor, row_slice(target), :],
            dst_ref=results[tensor].at[:, head_slice(me, head)],
            send_sem=back_send.at[0],
            recv_sem=back_recv.at[0],
            device_id=device_of(target),
            device_id_type=MESH,
        )

    def copy_share():
        return pltpu.make_async_remote_copy(
            src_ref=group_buf,
            dst_ref=group_buf,
            send_sem=share_send.at[0],
            recv_sem=share_recv.at[0],
            device_id=(dp, me * SEQS_CTX + 1 - core),
            device_id_type=MESH,
        )

    def copy_places(target):
        return pltpu.make_async_remote_copy(
            src_ref=positions,
            dst_ref=places.at[me],
            send_sem=place_send.at[0],
            recv_sem=place_recv.at[0],
            device_id=device_of(target),
            device_id_type=MESH,
        )

    def copy_plane(index):
        return pltpu.make_async_remote_copy(
            src_ref=gain_part.at[index],
            dst_ref=plane_buf.at[index],
            send_sem=plane_send.at[0],
            recv_sem=plane_recv.at[index],
            device_id=plane_device(bits[index]),
            device_id_type=MESH,
        )

    def copy_group(target):
        return pltpu.make_async_remote_copy(
            src_ref=gain_part.at[len(bits)],
            dst_ref=group_buf.at[me],
            send_sem=group_send.at[0],
            recv_sem=group_recv.at[0],
            device_id=device_of(target),
            device_id_type=MESH,
        )

    def waiter(part, send, receive):
        return pltpu.make_async_remote_copy(
            src_ref=part,
            dst_ref=part,
            send_sem=send.at[0],
            recv_sem=receive,
            device_id=device_of(inner),
            device_id_type=MESH,
        )

    elsewhere = pl.ds(0, (members - 1) * rows)
    all_in = waiter(in_buf.at[:, :, elsewhere, :], in_send, in_recv.at[0])
    all_back = waiter(out_buf.at[:, :, elsewhere, :], back_send, back_recv.at[0])
    all_places = waiter(places.at[pl.ds(0, members - 1)], place_send, place_recv.at[0])
    all_group = waiter(group_buf.at[pl.ds(0, members - 1)], group_send, group_recv.at[0])

    def signal(semaphore, device):
        pl.semaphore_signal(semaphore, 1, device_id=device, device_id_type=MESH)

    barrier = pltpu.get_barrier_semaphore()

    @pl.when(middle == 1)
    def _():
        signal(barrier, device_of(inner))

    @pl.when(spot > 0)
    def _():
        signal(barrier, device_of(outer))

    @pl.when(spot == 0)
    def _():
        for bit in bits:
            signal(barrier, plane_device(bit))

    pl.semaphore_wait(barrier, 1 + (half - spot) // half * len(bits))

    early = min(EARLY, per_device)

    def start_inner(head, carry):
        for tensor in range(4):
            copy_in(head, tensor, inner).start()
        return carry

    copy_places(inner).start()
    lax.fori_loop(0, early, start_inner, 0)

    def start_own(head, carry):
        for tensor in range(4):
            own_in(head, tensor).start()
        return carry

    small_copies = [
        pltpu.make_async_copy(positions, places.at[me], place_recv.at[0]),
        pltpu.make_async_copy(span_start_in, spans.at[0], small_sem.at[0]),
        pltpu.make_async_copy(span_length_in, spans.at[1], small_sem.at[0]),
        pltpu.make_async_copy(query_gain_in, gains.at[0], small_sem.at[1]),
        pltpu.make_async_copy(key_gain_in, gains.at[1], small_sem.at[1]),
    ]
    for copy in small_copies:
        copy.start()
    lax.fori_loop(0, per_device, start_own, 0)

    @pl.when(spot > 0)
    def _():
        pl.semaphore_wait(ready.at[0], 1)

    @pl.when(middle == 0)
    def _():
        signal(ready.at[0], device_of(inner))
        pl.semaphore_wait(ready.at[1], 1)

    @pl.when(middle == 1)
    def _():
        signal(ready.at[1], device_of(inner))
        pl.semaphore_wait(ready.at[1], 1)

    @pl.when(spot > 0)
    def _():
        signal(ready.at[1], device_of(outer))

    @pl.when(spot == 0)
    def _():
        for bit in bits:
            signal(ready.at[2], plane_device(bit))

    for target in others:
        copy_places(target).start()

    def start_others(head, carry):
        for target in others:
            for tensor in range(4):
                copy_in(head, tensor, target).start()
        return carry

    def start_all(head, carry):
        for target in targets:
            for tensor in range(4):
                copy_in(head, tensor, target).start()
        return carry

    lax.fori_loop(0, early, start_others, 0)
    lax.fori_loop(early, per_device, start_all, 0)

    pltpu.make_async_copy(spans, spans, small_sem.at[0]).wait()
    pltpu.make_async_copy(gains, gains, small_sem.at[1]).wait()
    waiter(places, place_send, place_recv.at[0]).wait_recv()

    starts = [spans[0, core, span] for span in range(spans.shape[2])]
    ends = [
        starts[span] + spans[1, core, span] for span in range(spans.shape[2])
    ]

    def labels_of(place):
        label = jnp.zeros_like(place)
        for span in range(len(starts)):
            inside = (place >= starts[span]) & (place < ends[span])
            label = label + jnp.where(inside, span + 1, 0)
        return label

    def fill_bias(member, carry):
        row_places = jnp.transpose(jnp.broadcast_to(places[member], (rows, rows)))
        row_labels = labels_of(row_places)
        for other in range(members):
            key_places = jnp.broadcast_to(places[other], (rows, rows))
            key_labels = labels_of(key_places)
            allowed = (key_places <= row_places) | (
                (row_labels == key_labels) & (row_labels > 0)
            )
            bias[row_slice(member), other * rows : (other + 1) * rows] = jnp.where(
                allowed, 0.0, masked_score
            )
        return carry

    lax.fori_loop(0, members, fill_bias, 0)

    block = min(tokens, 256)

    def one_head(head, carry):
        waiter(in_buf.at[head], in_send, in_recv.at[head]).wait_recv()
        gain_q = gains[0, pl.ds(me * per_device + head, 1), :]
        gain_k = gains[1, pl.ds(me * per_device + head, 1), :]
        key_unit, key_inverse = unit_of(in_buf[head, 1])
        key_normed[...] = (key_unit * gain_k).astype(jnp.bfloat16)
        key_total[...] = jnp.zeros_like(key_total)
        value_total[...] = jnp.zeros_like(value_total)

        def one_block(index, query_part):
            here = pl.ds(pl.multiple_of(index * block, block), block)
            unit, inverse = unit_of(in_buf[head, 0, here, :])
            normed = (unit * gain_q).astype(jnp.bfloat16)
            values = in_buf[head, 2]
            grads = in_buf[head, 3, here, :]
            scores = dot(normed, key_normed[...], 1, 1) * scale + bias[here, :]
            row_max = jnp.max(scores, axis=-1, keepdims=True)
            powers = jnp.exp(scores - row_max)
            probs = powers * (1.0 / jnp.sum(powers, axis=-1, keepdims=True))
            weights = probs.astype(jnp.bfloat16)
            output = dot(weights, values, 1, 0).astype(jnp.bfloat16)
            out_buf[head, 0, here, :] = output
            delta = jnp.sum(
                output.astype(jnp.float32) * grads.astype(jnp.float32), axis=-1, keepdims=True
            )
            value_total[...] += dot(weights, grads, 0, 0)
            prob_grads = dot(grads, values, 1, 1)
            score_grads = (probs * (prob_grads - delta)).astype(jnp.bfloat16)
            grad_query = dot(score_grads, key_normed[...], 1, 0) * scale
            key_total[...] += dot(score_grads, normed, 0, 0)
            raw_grad, part = norm_backward(grad_query, unit, inverse, gain_q)
            out_buf[head, 1, here, :] = raw_grad
            return query_part + part

        query_part = jnp.zeros((1, HEAD), jnp.float32)
        if tokens // block <= 2:
            for index in range(tokens // block):
                query_part = one_block(index, query_part)
        else:
            query_part = lax.fori_loop(0, tokens // block, one_block, query_part)
        raw_grad, key_part = norm_backward(key_total[...] * scale, key_unit, key_inverse, gain_k)
        out_buf[head, 2] = raw_grad
        out_buf[head, 3] = value_total[...].astype(jnp.bfloat16)
        gain_part[0, pl.ds(head, 1), :] = query_part
        gain_part[0, pl.ds(per_device + head, 1), :] = key_part
        for tensor in range(4):
            results[tensor][:, head_slice(me, head)] = out_buf[head, tensor, row_slice(me), :]

        @pl.when(head < per_device - 1)
        def _():
            start_back(head)

        return carry

    def start_back_to(head, chosen):
        for target in chosen:
            for tensor in range(4):
                copy_back(head, tensor, target).start()

    def start_back(head):
        start_back_to(head, others)

        @pl.when(head > 0)
        def _():
            start_back_to(head - 1, [inner])

    lax.fori_loop(0, per_device, one_head, 0)
    start_back_to(per_device - 1, others)

    @pl.when(spot == 0)
    def _():
        pl.semaphore_wait(ready.at[2], len(bits))

    @pl.when(spot > 0)
    def _():
        pl.semaphore_wait(ready.at[3], 1)

    @pl.when(middle == 0)
    def _():
        signal(ready.at[3], device_of(inner))

    for index in range(len(bits)):
        copy_plane(index).start()
        copy_plane(index).wait_recv()
        gain_part[index + 1] = gain_part[index] + plane_buf[index]
    @pl.when(core == 1)
    def _():
        group_buf[me] = gain_part[len(bits)]
        for target in targets:
            copy_group(target).start()

    if per_device > 1:
        start_back_to(per_device - 2, [inner])
    start_back_to(per_device - 1, [inner])

    @pl.when(core == 1)
    def _():
        all_group.wait_recv()
        copy_share().start()

    @pl.when(core == 0)
    def _():
        copy_share().wait_recv()

    for member in range(members):
        for head in range(per_device):
            at = (member * per_device + head) * HEAD
            gain_ref[0:1, at : at + HEAD] = group_buf[member, head : head + 1, :]
            gain_ref[1:2, at : at + HEAD] = group_buf[
                member, per_device + head : per_device + head + 1, :
            ]

    waiter(plane_buf, plane_send, plane_recv.at[0]).wait_send()

    all_in.wait_send()
    all_places.wait_send()

    @pl.when(core == 1)
    def _():
        all_group.wait_send()
        copy_share().wait_send()

    all_back.wait_send()
    all_back.wait_recv()


def place_results(*refs):
    count = len(refs) // 2
    copies = [
        pltpu.make_async_copy(refs[index], refs[count + index], refs[-1].at[index])
        for index in range(count)
    ]
    for copy in copies:
        copy.start()
    for copy in copies:
        copy.wait()


def body(
    members,
    dp_count,
    query_rows,
    key_rows,
    value_rows,
    cotangent,
    query_gain,
    key_gain,
    positions,
    span_start,
    span_length,
):
    rows, width = query_rows.shape
    heads = width // HEAD
    per_device = heads // members
    tokens = members * rows
    rounds = (dp_count * SEQS_CTX).bit_length() - 1
    hbm = pl.BlockSpec(memory_space=pltpu.HBM)
    vmem = pl.BlockSpec(memory_space=pltpu.VMEM)
    wide = pltpu.VMEM((rows, width), jnp.bfloat16)
    dma = pltpu.SemaphoreType.DMA
    held = pl.pallas_call(
        functools.partial(kernel, members, dp_count, per_device, rows),
        out_shape=(wide, wide, wide, wide, pltpu.VMEM((2, width), jnp.float32)),
        in_specs=[hbm] * 9,
        out_specs=(vmem, vmem, vmem, vmem, vmem),
        scratch_shapes=[
            pltpu.VMEM((2, heads, HEAD), jnp.float32),
            pltpu.SMEM((2,) + span_start.shape, jnp.int32),
            dma((2,)),
            pltpu.VMEM((per_device, 4, tokens, HEAD), jnp.bfloat16),
            pltpu.VMEM((per_device, 4, tokens, HEAD), jnp.bfloat16),
            pltpu.VMEM((tokens, tokens), jnp.float32),
            pltpu.VMEM((tokens, HEAD), jnp.bfloat16),
            pltpu.VMEM((tokens, HEAD), jnp.float32),
            pltpu.VMEM((tokens, HEAD), jnp.float32),
            pltpu.VMEM((members, 1, rows), jnp.int32),
            pltpu.VMEM((rounds + 1, 2 * per_device, HEAD), jnp.float32),
            pltpu.VMEM((rounds, 2 * per_device, HEAD), jnp.float32),
            pltpu.VMEM((members, 2 * per_device, HEAD), jnp.float32),
            pltpu.SemaphoreType.REGULAR((4,)),
            dma((1,)),
            dma((per_device,)),
            dma((1,)),
            dma((1,)),
            dma((1,)),
            dma((1,)),
            dma((1,)),
            dma((rounds,)),
            dma((1,)),
            dma((1,)),
            dma((1,)),
            dma((1,)),
        ],
        compiler_params=pltpu.CompilerParams(
            collective_id=0, has_side_effects=True, vmem_limit_bytes=123 * 512 * 1024
        ),
    )(
        query_rows,
        key_rows,
        value_rows,
        cotangent,
        query_gain.reshape(heads, HEAD),
        key_gain.reshape(heads, HEAD),
        positions.reshape(1, rows),
        span_start,
        span_length,
    )
    return pl.pallas_call(
        place_results,
        out_shape=tuple(jax.ShapeDtypeStruct(array.shape, array.dtype) for array in held),
        in_specs=[pl.BlockSpec(memory_space=pl.ANY)] * 5,
        out_specs=(pl.BlockSpec(memory_space=pltpu.HBM),) * 5,
        scratch_shapes=[dma((5,))],
        compiler_params=pltpu.CompilerParams(vmem_limit_bytes=1024 * 1024),
    )(*held)


def solution(mesh):
    row_spec = P(("dp", "ctx"), None)
    in_specs = (
        row_spec,
        row_spec,
        row_spec,
        row_spec,
        P(),
        P(),
        P(("dp", "ctx")),
        P("dp", None),
        P("dp", None),
    )
    out_specs = (row_spec, row_spec, row_spec, row_spec, P())
    members = mesh.shape["ctx"] // SEQS_CTX
    return jax.shard_map(
        functools.partial(body, members, mesh.shape["dp"]),
        mesh=mesh,
        in_specs=in_specs,
        out_specs=out_specs,
        check_vma=False,
    )
```

```python
import functools

import jax
import jax.numpy as jnp
from jax import lax
from jax.experimental import pallas as pl
from jax.experimental.pallas import tpu as pltpu
from jax.sharding import PartitionSpec as P

HEAD = 128
SEQS_CTX = 2
EARLY = 2

epsilon = 1e-05
masked_score = -1e30
MESH = pl.DeviceIdType.MESH


def flip(index, distance, count):
    result = index
    bit = 1
    while bit < count:
        if distance & bit:
            result = result + bit - 2 * bit * ((index // bit) % 2)
        bit *= 2
    return result


def unit_of(raw):
    values = raw.astype(jnp.float32)
    inverse = lax.rsqrt(jnp.mean(values * values, axis=-1, keepdims=True) + epsilon)
    return values * inverse, inverse


def norm_backward(grad_normed, unit, inverse, gain):
    grad_unit = grad_normed * gain
    projected = jnp.mean(grad_unit * unit, axis=-1, keepdims=True)
    grad_raw = inverse * (grad_unit - unit * projected)
    return grad_raw.astype(jnp.bfloat16), jnp.sum(grad_normed * unit, axis=0, keepdims=True)


def dot(left, right, left_axis, right_axis):
    return lax.dot_general(
        left,
        right,
        (((left_axis,), (right_axis,)), ((), ())),
        preferred_element_type=jnp.float32,
    )


def kernel(
    members,
    dp_count,
    per_device,
    rows,
    query_in,
    key_in,
    value_in,
    cotangent_in,
    query_gain_in,
    key_gain_in,
    positions,
    span_start_in,
    span_length_in,
    out_ref,
    query_grad_ref,
    key_grad_ref,
    value_grad_ref,
    gain_ref,
    gains,
    spans,
    small_sem,
    in_buf,
    out_buf,
    bias,
    key_normed,
    key_total,
    value_total,
    places,
    gain_part,
    plane_buf,
    group_buf,
    ready,
    in_send,
    in_recv,
    back_send,
    back_recv,
    place_send,
    place_recv,
    plane_send,
    plane_recv,
    group_send,
    group_recv,
    share_send,
    share_recv,
):
    dp = lax.axis_index("dp")
    ctx = lax.axis_index("ctx")
    me = ctx // SEQS_CTX
    core = ctx % SEQS_CTX
    tokens = members * rows
    plane = dp_count * SEQS_CTX
    own = dp * SEQS_CTX + core
    sources = (query_in, key_in, value_in, cotangent_in)
    results = (out_ref, query_grad_ref, key_grad_ref, value_grad_ref)
    scale = HEAD ** (-0.5)
    half = members // 2
    upper = me // half

    def mirror(index):
        return index + upper * (members - 1 - 2 * index)

    spot = mirror(me)
    middle = (spot + 1) // half
    inner = mirror(spot + 1)
    outer = mirror(spot - 1)
    others = [mirror(members - 1 - step) for step in range(half - 1)]
    if half > 1:
        others.append(mirror(half + middle * ((spot + 1) % half - half)))
    others += [mirror((spot + step) % half) for step in range(2, half)]
    targets = others + [inner]

    def row_slice(member):
        return pl.ds(pl.multiple_of(member * rows, rows), rows)

    def head_slice(member, head):
        return pl.ds(pl.multiple_of((member * per_device + head) * HEAD, HEAD), HEAD)

    def device_of(member):
        return (dp, member * SEQS_CTX + core)

    def plane_device(bit):
        other = flip(own, bit, plane)
        return (other // SEQS_CTX, me * SEQS_CTX + other % SEQS_CTX)

    bits = [1 << index for index in range(plane.bit_length() - 1)]

    def own_in(head, tensor):
        return pltpu.make_async_copy(
            sources[tensor].at[:, head_slice(me, head)],
            in_buf.at[head, tensor, row_slice(me), :],
            in_recv.at[head],
        )

    def copy_in(head, tensor, target):
        return pltpu.make_async_remote_copy(
            src_ref=sources[tensor].at[:, head_slice(target, head)],
            dst_ref=in_buf.at[head, tensor, row_slice(me), :],
            send_sem=in_send.at[0],
            recv_sem=in_recv.at[head],
            device_id=device_of(target),
            device_id_type=MESH,
        )

    def copy_back(head, tensor, target):
        return pltpu.make_async_remote_copy(
            src_ref=out_buf.at[head, tensor, row_slice(target), :],
            dst_ref=results[tensor].at[:, head_slice(me, head)],
            send_sem=back_send.at[0],
            recv_sem=back_recv.at[0],
            device_id=device_of(target),
            device_id_type=MESH,
        )

    def copy_share():
        return pltpu.make_async_remote_copy(
            src_ref=group_buf,
            dst_ref=group_buf,
            send_sem=share_send.at[0],
            recv_sem=share_recv.at[0],
            device_id=(dp, me * SEQS_CTX + 1 - core),
            device_id_type=MESH,
        )

    def copy_places(target):
        return pltpu.make_async_remote_copy(
            src_ref=positions,
            dst_ref=places.at[me],
            send_sem=place_send.at[0],
            recv_sem=place_recv.at[0],
            device_id=device_of(target),
            device_id_type=MESH,
        )

    def copy_plane(index):
        return pltpu.make_async_remote_copy(
            src_ref=gain_part.at[index],
            dst_ref=plane_buf.at[index],
            send_sem=plane_send.at[0],
            recv_sem=plane_recv.at[index],
            device_id=plane_device(bits[index]),
            device_id_type=MESH,
        )

    def copy_group(target):
        return pltpu.make_async_remote_copy(
            src_ref=gain_part.at[len(bits)],
            dst_ref=group_buf.at[me],
            send_sem=group_send.at[0],
            recv_sem=group_recv.at[0],
            device_id=device_of(target),
            device_id_type=MESH,
        )

    def waiter(part, send, receive):
        return pltpu.make_async_remote_copy(
            src_ref=part,
            dst_ref=part,
            send_sem=send.at[0],
            recv_sem=receive,
            device_id=device_of(inner),
            device_id_type=MESH,
        )

    elsewhere = pl.ds(0, (members - 1) * rows)
    all_in = waiter(in_buf.at[:, :, elsewhere, :], in_send, in_recv.at[0])
    all_back = waiter(out_buf.at[:, :, elsewhere, :], back_send, back_recv.at[0])
    all_places = waiter(places.at[pl.ds(0, members - 1)], place_send, place_recv.at[0])
    all_group = waiter(group_buf.at[pl.ds(0, members - 1)], group_send, group_recv.at[0])

    def signal(semaphore, device):
        pl.semaphore_signal(semaphore, 1, device_id=device, device_id_type=MESH)

    barrier = pltpu.get_barrier_semaphore()

    @pl.when(middle == 1)
    def _():
        signal(barrier, device_of(inner))

    @pl.when(spot > 0)
    def _():
        signal(barrier, device_of(outer))

    @pl.when(spot == 0)
    def _():
        for bit in bits:
            signal(barrier, plane_device(bit))

    pl.semaphore_wait(barrier, 1 + (half - spot) // half * len(bits))

    early = min(EARLY, per_device)

    def start_inner(head, carry):
        for tensor in range(4):
            copy_in(head, tensor, inner).start()
        return carry

    lax.fori_loop(0, early, start_inner, 0)
    copy_places(inner).start()

    def start_own(head, carry):
        for tensor in range(4):
            own_in(head, tensor).start()
        return carry

    small_copies = [
        pltpu.make_async_copy(positions, places.at[me], place_recv.at[0]),
        pltpu.make_async_copy(span_start_in, spans.at[0], small_sem.at[0]),
        pltpu.make_async_copy(span_length_in, spans.at[1], small_sem.at[0]),
        pltpu.make_async_copy(query_gain_in, gains.at[0], small_sem.at[1]),
        pltpu.make_async_copy(key_gain_in, gains.at[1], small_sem.at[1]),
    ]
    for copy in small_copies:
        copy.start()
    lax.fori_loop(0, per_device, start_own, 0)

    @pl.when(spot > 0)
    def _():
        pl.semaphore_wait(ready.at[0], 1)

    @pl.when(middle == 0)
    def _():
        signal(ready.at[0], device_of(inner))
        pl.semaphore_wait(ready.at[1], 1)

    @pl.when(middle == 1)
    def _():
        signal(ready.at[1], device_of(inner))
        pl.semaphore_wait(ready.at[1], 1)

    @pl.when(spot > 0)
    def _():
        signal(ready.at[1], device_of(outer))

    @pl.when(spot == 0)
    def _():
        for bit in bits:
            signal(ready.at[2], plane_device(bit))

    for target in others:
        copy_places(target).start()

    def start_others(head, carry):
        for target in others:
            for tensor in range(4):
                copy_in(head, tensor, target).start()
        return carry

    def start_all(head, carry):
        for target in targets:
            for tensor in range(4):
                copy_in(head, tensor, target).start()
        return carry

    lax.fori_loop(0, early, start_others, 0)
    lax.fori_loop(early, per_device, start_all, 0)

    pltpu.make_async_copy(spans, spans, small_sem.at[0]).wait()
    pltpu.make_async_copy(gains, gains, small_sem.at[1]).wait()
    waiter(places, place_send, place_recv.at[0]).wait_recv()

    starts = [spans[0, core, span] for span in range(spans.shape[2])]
    ends = [
        starts[span] + spans[1, core, span] for span in range(spans.shape[2])
    ]

    def labels_of(place):
        label = jnp.zeros_like(place)
        for span in range(len(starts)):
            inside = (place >= starts[span]) & (place < ends[span])
            label = label + jnp.where(inside, span + 1, 0)
        return label

    def fill_bias(member, carry):
        row_places = jnp.transpose(jnp.broadcast_to(places[member], (rows, rows)))
        row_labels = labels_of(row_places)
        for other in range(members):
            key_places = jnp.broadcast_to(places[other], (rows, rows))
            key_labels = labels_of(key_places)
            allowed = (key_places <= row_places) | (
                (row_labels == key_labels) & (row_labels > 0)
            )
            bias[row_slice(member), other * rows : (other + 1) * rows] = jnp.where(
                allowed, 0.0, masked_score
            )
        return carry

    lax.fori_loop(0, members, fill_bias, 0)

    block = min(tokens, 256)

    def one_head(head, carry):
        waiter(in_buf.at[head], in_send, in_recv.at[head]).wait_recv()
        gain_q = gains[0, pl.ds(me * per_device + head, 1), :]
        gain_k = gains[1, pl.ds(me * per_device + head, 1), :]
        key_unit, key_inverse = unit_of(in_buf[head, 1])
        key_normed[...] = (key_unit * gain_k).astype(jnp.bfloat16)
        key_total[...] = jnp.zeros_like(key_total)
        value_total[...] = jnp.zeros_like(value_total)

        def one_block(index, query_part):
            here = pl.ds(pl.multiple_of(index * block, block), block)
            unit, inverse = unit_of(in_buf[head, 0, here, :])
            normed = (unit * gain_q).astype(jnp.bfloat16)
            values = in_buf[head, 2]
            grads = in_buf[head, 3, here, :]
            scores = dot(normed, key_normed[...], 1, 1) * scale + bias[here, :]
            row_max = jnp.max(scores, axis=-1, keepdims=True)
            powers = jnp.exp(scores - row_max)
            probs = powers * (1.0 / jnp.sum(powers, axis=-1, keepdims=True))
            weights = probs.astype(jnp.bfloat16)
            output = dot(weights, values, 1, 0).astype(jnp.bfloat16)
            out_buf[head, 0, here, :] = output
            delta = jnp.sum(
                output.astype(jnp.float32) * grads.astype(jnp.float32), axis=-1, keepdims=True
            )
            value_total[...] += dot(weights, grads, 0, 0)
            prob_grads = dot(grads, values, 1, 1)
            score_grads = (probs * (prob_grads - delta)).astype(jnp.bfloat16)
            grad_query = dot(score_grads, key_normed[...], 1, 0) * scale
            key_total[...] += dot(score_grads, normed, 0, 0)
            raw_grad, part = norm_backward(grad_query, unit, inverse, gain_q)
            out_buf[head, 1, here, :] = raw_grad
            return query_part + part

        query_part = jnp.zeros((1, HEAD), jnp.float32)
        if tokens // block <= 2:
            for index in range(tokens // block):
                query_part = one_block(index, query_part)
        else:
            query_part = lax.fori_loop(0, tokens // block, one_block, query_part)
        raw_grad, key_part = norm_backward(key_total[...] * scale, key_unit, key_inverse, gain_k)
        out_buf[head, 2] = raw_grad
        out_buf[head, 3] = value_total[...].astype(jnp.bfloat16)
        gain_part[0, pl.ds(head, 1), :] = query_part
        gain_part[0, pl.ds(per_device + head, 1), :] = key_part
        for tensor in range(4):
            results[tensor][:, head_slice(me, head)] = out_buf[head, tensor, row_slice(me), :]

        @pl.when(head < per_device - 1)
        def _():
            start_back(head)

        return carry

    def start_back_to(head, chosen):
        for target in chosen:
            for tensor in range(4):
                copy_back(head, tensor, target).start()

    def start_back(head):
        start_back_to(head, others)

        @pl.when(head > 0)
        def _():
            start_back_to(head - 1, [inner])

    lax.fori_loop(0, per_device, one_head, 0)
    start_back_to(per_device - 1, others)

    @pl.when(spot == 0)
    def _():
        pl.semaphore_wait(ready.at[2], len(bits))

    @pl.when(spot > 0)
    def _():
        pl.semaphore_wait(ready.at[3], 1)

    @pl.when(middle == 0)
    def _():
        signal(ready.at[3], device_of(inner))

    for index in range(len(bits)):
        copy_plane(index).start()
        copy_plane(index).wait_recv()
        gain_part[index + 1] = gain_part[index] + plane_buf[index]
    @pl.when(core == 1)
    def _():
        group_buf[me] = gain_part[len(bits)]
        for target in targets:
            copy_group(target).start()

    if per_device > 1:
        start_back_to(per_device - 2, [inner])
    start_back_to(per_device - 1, [inner])

    @pl.when(core == 1)
    def _():
        all_group.wait_recv()
        copy_share().start()

    @pl.when(core == 0)
    def _():
        copy_share().wait_recv()

    for member in range(members):
        for head in range(per_device):
            at = (member * per_device + head) * HEAD
            gain_ref[0:1, at : at + HEAD] = group_buf[member, head : head + 1, :]
            gain_ref[1:2, at : at + HEAD] = group_buf[
                member, per_device + head : per_device + head + 1, :
            ]

    waiter(plane_buf, plane_send, plane_recv.at[0]).wait_send()

    all_in.wait_send()
    all_places.wait_send()

    @pl.when(core == 1)
    def _():
        all_group.wait_send()
        copy_share().wait_send()

    all_back.wait_send()
    all_back.wait_recv()


def place_results(*refs):
    count = len(refs) // 2
    copies = [
        pltpu.make_async_copy(refs[index], refs[count + index], refs[-1].at[index])
        for index in range(count)
    ]
    for copy in copies:
        copy.start()
    for copy in copies:
        copy.wait()


def body(
    members,
    dp_count,
    query_rows,
    key_rows,
    value_rows,
    cotangent,
    query_gain,
    key_gain,
    positions,
    span_start,
    span_length,
):
    rows, width = query_rows.shape
    heads = width // HEAD
    per_device = heads // members
    tokens = members * rows
    rounds = (dp_count * SEQS_CTX).bit_length() - 1
    hbm = pl.BlockSpec(memory_space=pltpu.HBM)
    vmem = pl.BlockSpec(memory_space=pltpu.VMEM)
    wide = pltpu.VMEM((rows, width), jnp.bfloat16)
    dma = pltpu.SemaphoreType.DMA
    held = pl.pallas_call(
        functools.partial(kernel, members, dp_count, per_device, rows),
        out_shape=(wide, wide, wide, wide, pltpu.VMEM((2, width), jnp.float32)),
        in_specs=[hbm] * 9,
        out_specs=(vmem, vmem, vmem, vmem, vmem),
        scratch_shapes=[
            pltpu.VMEM((2, heads, HEAD), jnp.float32),
            pltpu.SMEM((2,) + span_start.shape, jnp.int32),
            dma((2,)),
            pltpu.VMEM((per_device, 4, tokens, HEAD), jnp.bfloat16),
            pltpu.VMEM((per_device, 4, tokens, HEAD), jnp.bfloat16),
            pltpu.VMEM((tokens, tokens), jnp.float32),
            pltpu.VMEM((tokens, HEAD), jnp.bfloat16),
            pltpu.VMEM((tokens, HEAD), jnp.float32),
            pltpu.VMEM((tokens, HEAD), jnp.float32),
            pltpu.VMEM((members, 1, rows), jnp.int32),
            pltpu.VMEM((rounds + 1, 2 * per_device, HEAD), jnp.float32),
            pltpu.VMEM((rounds, 2 * per_device, HEAD), jnp.float32),
            pltpu.VMEM((members, 2 * per_device, HEAD), jnp.float32),
            pltpu.SemaphoreType.REGULAR((4,)),
            dma((1,)),
            dma((per_device,)),
            dma((1,)),
            dma((1,)),
            dma((1,)),
            dma((1,)),
            dma((1,)),
            dma((rounds,)),
            dma((1,)),
            dma((1,)),
            dma((1,)),
            dma((1,)),
        ],
        compiler_params=pltpu.CompilerParams(
            collective_id=0, has_side_effects=True, vmem_limit_bytes=123 * 512 * 1024
        ),
    )(
        query_rows,
        key_rows,
        value_rows,
        cotangent,
        query_gain.reshape(heads, HEAD),
        key_gain.reshape(heads, HEAD),
        positions.reshape(1, rows),
        span_start,
        span_length,
    )
    return pl.pallas_call(
        place_results,
        out_shape=tuple(jax.ShapeDtypeStruct(array.shape, array.dtype) for array in held),
        in_specs=[pl.BlockSpec(memory_space=pl.ANY)] * 5,
        out_specs=(pl.BlockSpec(memory_space=pltpu.HBM),) * 5,
        scratch_shapes=[dma((5,))],
        compiler_params=pltpu.CompilerParams(vmem_limit_bytes=1024 * 1024),
    )(*held)


def solution(mesh):
    row_spec = P(("dp", "ctx"), None)
    in_specs = (
        row_spec,
        row_spec,
        row_spec,
        row_spec,
        P(),
        P(),
        P(("dp", "ctx")),
        P("dp", None),
        P("dp", None),
    )
    out_specs = (row_spec, row_spec, row_spec, row_spec, P())
    members = mesh.shape["ctx"] // SEQS_CTX
    return jax.shard_map(
        functools.partial(body, members, mesh.shape["dp"]),
        mesh=mesh,
        in_specs=in_specs,
        out_specs=out_specs,
        check_vma=False,
    )
```
